512 devices in a mesh: grp: 2 (over y), lon: 32 (over z), view: 8 (over x, core).
Axes of the slice: x: 4, y: 2, z: 32, core: 2. Of those that a mesh axis runs over, the one named last changes fastest.
The devices are a block of a 4x8x32 slice.
Arguments:
- light_field: bfloat16 [128, 8, 1024, 128], P(('grp', 'view'), None, 'lon'), parts along dimension 0, may hold values from -6 to 6
- spatial_weights: bfloat16 [3, 3, 3, 128, 128], replicated, may hold values from -0.1875 to 0.1875
- spatial_offsets: float32 [3, 128], replicated, may hold values from -3 to 3
- angular_weight: bfloat16 [3, 3, 128, 128], replicated, may hold values from -0.1875 to 0.1875
- angular_offset: float32 [128], replicated, may hold values from -3 to 3
Outputs:
- refined: bfloat16 [128, 8, 1024, 128], P(('grp', 'view'), None, 'lon'), parts along dimension 0
The draws below stay inside these ranges and needn't reach their ends.
There are 2 independent parts, one for each index of `grp`. The reference program is written for one: setup_inputs(seed, part) draws one part's arguments, and reference() takes and returns one part's arrays. A program takes and returns all parts, laid end to end along the dimension named above; an argument that names none is the same for every part. Nothing has to cross between parts.
All inputs are finite; a program needn't handle non-finite values.
Results may differ from the reference program's by a relative error of at most 0.0047.
Values may be sent and summed in bfloat16 or wider, within the bound.
No kernel may reach another device: no remote copies, remote signals or barrier semaphores. Data moves between devices by JAX's collectives and lax.ppermute only.
A program may use at most 64 MiB of HBM per device.

```python
import jax
import jax.numpy as jnp
from jax import lax

C = 128
ANG = 8
LAYERS = 3
VIEWS = 64
ROWS = 8
COLS = 1024


def shard_levels(key, extent, shards, smallest, high):
    def one(position, blocks):
        draws = jax.random.uniform(jax.random.fold_in(jax.random.fold_in(key, 6), position), (blocks,), jnp.float32, smallest / len(shards), high / len(shards))
        return jnp.repeat(jnp.exp(draws), extent[position] // blocks).reshape((-1,) + (1,) * (len(extent) - position - 1))

    level = one(*shards[0])
    for cut in shards[1:]:
        level = level * one(*cut)
    return level


def gaussian(own_key, dims, deviation, limit, cuts=(), held_as=jnp.bfloat16):
    entries = deviation * jax.random.normal(own_key, dims, jnp.float32)
    if cuts:
        entries = entries * shard_levels(own_key, dims, cuts, -0.22, 0.18)
    return jnp.clip(entries, -limit, limit).astype(held_as)


def setup_inputs(seed: int = 0, part: int = 0) -> dict:
    seeds = jax.random.split(jax.random.key(seed), 6)
    part_splits = jax.random.split(jax.random.fold_in(seeds[5], part), 6)
    light_field = gaussian(part_splits[0], (VIEWS, ROWS, COLS, C), 1.0, 6.0, ((0, 8), (2, 32)))
    spatial_weights = gaussian(seeds[1], (LAYERS, 3, 3, C, C), (9 * C) ** -0.5, 0.1875)
    spatial_offsets = gaussian(seeds[2], (LAYERS, C), 0.5, 3.0, (), jnp.float32)
    angular_weight = gaussian(seeds[3], (3, 3, C, C), (9 * C) ** -0.5, 0.1875)
    angular_offset = gaussian(seeds[4], (C,), 0.5, 3.0, (), jnp.float32)
    return {"light_field": light_field, "spatial_weights": spatial_weights, "spatial_offsets": spatial_offsets, "angular_weight": angular_weight, "angular_offset": angular_offset}


def spatial_layer(hidden, weight, offset):
    rows, cols, chans = hidden.shape
    padded = jnp.pad(hidden, ((1, 1), (0, 0), (0, 0)))
    padded = jnp.concatenate([padded[:, -1:], padded, padded[:, :1]], axis=1)
    total = jnp.zeros((rows * cols, chans), jnp.float32)
    for row_tap in range(3):
        for col_tap in range(3):
            window = padded[row_tap:row_tap + rows, col_tap:col_tap + cols].reshape(-1, chans)
            total = total + jnp.dot(window, weight[row_tap, col_tap], preferred_element_type=jnp.float32)
    total = total.reshape(rows, cols, chans) + offset
    return jax.nn.gelu(total, approximate=True).astype(jnp.bfloat16)


def reference(light_field, spatial_weights, spatial_offsets, angular_weight, angular_offset):
    hidden = light_field
    for layer_index in range(LAYERS):
        weight = spatial_weights[layer_index]
        offset = spatial_offsets[layer_index]
        hidden = lax.map(lambda single: spatial_layer(single, weight, offset), hidden)
    chans = hidden.shape[-1]
    views_grid = hidden.reshape(ANG, ANG, -1, chans)
    padded = jnp.pad(views_grid, ((1, 1), (1, 1), (0, 0), (0, 0)))
    total = jnp.zeros((views_grid.shape[0] * ANG * views_grid.shape[2], chans), jnp.float32)
    for row_tap in range(3):
        for col_tap in range(3):
            window = padded[row_tap:row_tap + ANG, col_tap:col_tap + ANG].reshape(-1, chans)
            total = total + jnp.dot(window, angular_weight[row_tap, col_tap], preferred_element_type=jnp.float32)
    angular = (total + angular_offset).astype(jnp.bfloat16)
    angular = lax.optimization_barrier(angular).reshape(light_field.shape)
    return (light_field.astype(jnp.float32) + angular.astype(jnp.float32)).astype(jnp.bfloat16)
```

```python
import functools

import jax
import jax.numpy as jnp
from jax import lax
from jax.experimental import pallas as pl
from jax.experimental.pallas import tpu as pltpu
from jax.sharding import PartitionSpec as P

EDGE = 4
HALO = 2 * EDGE


def gelu(t):
    half = 0.5 * t
    return half + half * jnp.tanh(t * (0.7978845608 + (0.7978845608 * 0.044715) * (t * t)))


def put_shifted(dst, row, cells, views, cols):
    for shift, moved in ((0, pltpu.roll(cells, 1, 1)), (1, cells), (2, pltpu.roll(cells, cols + HALO - 1, 1))):
        chans = cells.shape[-1]
        dst[shift, row, : views * cols] = moved[:, :cols].reshape(views * cols, chans).astype(dst.dtype)
        dst[shift, row, views * cols :] = moved[:, cols:].reshape(views * HALO, chans).astype(dst.dtype)


def hidden_kernel(side_ref, field_ref, near_ref, far_ref, weight_ref, offset_ref, out_ref, even, odd):
    views, rows, cols, chans = field_ref.shape
    layers = weight_ref.shape[0]
    own = views * cols
    for buf in (even, odd):
        for shift in range(3):
            for row in (0, rows + 1):
                buf[shift, row] = jnp.zeros(buf.shape[2:], buf.dtype)
    first = side_ref[0] == 0
    for row in range(rows):
        near = near_ref[:, row].astype(jnp.float32)
        far = far_ref[:, row].astype(jnp.float32)
        right = jnp.where(first, near, far)
        left = jnp.where(first, far, near)
        cells = jnp.concatenate([field_ref[:, row].astype(jnp.float32), right, left], axis=1)
        put_shifted(even, row + 1, cells, views, cols)
    blank = jnp.zeros((chans, chans), weight_ref.dtype)
    bufs = (even, odd)
    for layer in range(layers):
        src, dst = bufs[layer % 2], bufs[(layer + 1) % 2]
        last = layer == layers - 1
        span = own if last else own + views * HALO
        weight = jnp.concatenate(
            [
                jnp.concatenate(
                    [weight_ref[layer, k, b] if k < 3 else blank, weight_ref[layer, k - 1, b] if k > 0 else blank],
                    axis=1,
                )
                for k in range(4)
                for b in range(3)
            ],
            axis=0,
        )
        offset = offset_ref[layer]
        for pair in range(rows // 2):
            stacked = jnp.concatenate(
                [src[b, 2 * pair + k, :span] for k in range(4) for b in range(3)], axis=1
            )
            total = jnp.dot(stacked, weight, preferred_element_type=jnp.float32)
            for r in range(2):
                value = gelu(total[:, r * chans : (r + 1) * chans] + offset)
                row = 2 * pair + r
                if last:
                    out_ref[row] = value.astype(out_ref.dtype)
                else:
                    cells = jnp.concatenate(
                        [value[:own].reshape(views, cols, chans), value[own:].reshape(views, HALO, chans)], axis=1
                    )
                    put_shifted(dst, row + 1, cells, views, cols)


def angular_kernel(side_ref, hidden_ref, far_ref, near_ref, weight_ref, offset_ref, field_ref, out_hbm, out, sems):
    views, rows, cols, chans = field_ref.shape
    even = side_ref[0] == 0
    far_tap = jnp.where(even, 0, 2)
    near_tap = 2 - far_tap
    sources = ((hidden_ref, 1), (near_ref, near_tap), (far_ref, far_tap))
    offset = offset_ref[...]
    blank = jnp.zeros((chans, chans), weight_ref.dtype)
    copies = []
    for pair in range(views // 2):
        stacked, weight = [], []
        for ref, tap in sources:
            for k in range(4):
                view = 2 * pair + k - 1
                if 0 <= view < views:
                    stacked.append(ref[:, view * cols : (view + 1) * cols].reshape(rows * cols, chans))
                    weight.append(
                        jnp.concatenate(
                            [weight_ref[tap, k] if k < 3 else blank, weight_ref[tap, k - 1] if k > 0 else blank],
                            axis=1,
                        )
                    )
        total = jnp.dot(
            jnp.concatenate(stacked, axis=1), jnp.concatenate(weight, axis=0), preferred_element_type=jnp.float32
        )
        for r in range(2):
            view = 2 * pair + r
            angular = (total[:, r * chans : (r + 1) * chans] + offset).astype(jnp.bfloat16)
            field = field_ref[view].reshape(rows * cols, chans).astype(jnp.float32)
            out[view] = (field + angular.astype(jnp.float32)).astype(out.dtype).reshape(rows, cols, chans)
        part = pl.ds(2 * pair, 2)
        copies.append(pltpu.make_async_copy(out.at[part], out_hbm.at[part], sems.at[pair]))
        copies[-1].start()
    for copy in copies:
        copy.wait()


VMEM = pl.BlockSpec(memory_space=pltpu.VMEM)
SMEM = pl.BlockSpec(memory_space=pltpu.SMEM)


def swap(cells, axis, start, count, closed):
    pairs = []
    for i in range(start, count, 2):
        j = i + 1
        if j < count or closed:
            pairs += [(i, j % count), (j % count, i)]
    return lax.ppermute(cells, axis, pairs)


def local(light_field, spatial_weights, spatial_offsets, angular_weight, angular_offset):
    views, rows, cols, chans = light_field.shape
    lon_count, view_count = lax.axis_size("lon"), lax.axis_size("view")
    lon_side = lax.rem(lax.axis_index("lon"), 2)
    view_side = lax.rem(lax.axis_index("view"), 2)
    head, tail = light_field[:, :, :EDGE], light_field[:, :, cols - EDGE :]
    far = swap(jnp.where(lon_side == 0, head, tail), "lon", 1, lon_count, True)
    near = swap(jnp.where(lon_side == 0, tail, head), "lon", 0, lon_count, True)
    span = views * (cols + HALO)
    hidden = pl.pallas_call(
        hidden_kernel,
        out_shape=jax.ShapeDtypeStruct((rows, views * cols, chans), jnp.bfloat16),
        in_specs=[SMEM, VMEM, VMEM, VMEM, VMEM, VMEM],
        out_specs=VMEM,
        scratch_shapes=[pltpu.VMEM((3, rows + 2, span, chans), jnp.bfloat16)] * 2,
        compiler_params=pltpu.CompilerParams(vmem_limit_bytes=24 * 2**20),
        name="hidden",
    )(lon_side[None], light_field, near, far, spatial_weights, spatial_offsets[:, None])
    far_rows = swap(hidden, "view", 1, view_count, False)
    near_rows = swap(hidden, "view", 0, view_count, False)
    return pl.pallas_call(
        angular_kernel,
        out_shape=jax.ShapeDtypeStruct(light_field.shape, jnp.bfloat16),
        in_specs=[SMEM, VMEM, VMEM, VMEM, VMEM, VMEM, VMEM],
        out_specs=pl.BlockSpec(memory_space=pl.ANY),
        scratch_shapes=[
            pltpu.VMEM(light_field.shape, jnp.bfloat16),
            pltpu.SemaphoreType.DMA((views // 2,)),
        ],
        compiler_params=pltpu.CompilerParams(vmem_limit_bytes=16 * 2**20),
        name="angular",
    )(view_side[None], hidden, far_rows, near_rows, angular_weight, angular_offset[None], light_field)


def solution(mesh):
    return jax.shard_map(
        local,
        mesh=mesh,
        in_specs=(P(("grp", "view"), None, "lon", None), P(), P(), P(), P()),
        out_specs=P(("grp", "view"), None, "lon", None),
        check_vma=False,
    )
```

```python
import jax
import jax.numpy as jnp
from jax import lax
from jax.experimental import pallas as pl
from jax.experimental.pallas import tpu as pltpu
from jax.sharding import PartitionSpec as P


EDGE = 4
TILE = 8
GROUPS = 4
VMEM = pl.BlockSpec(memory_space=pltpu.VMEM)
SMEM = pl.BlockSpec(memory_space=pltpu.SMEM)
HBM = pl.BlockSpec(memory_space=pl.ANY)


def gelu(t):
    half = 0.5 * t
    return half + half * jnp.tanh(t * (0.7978845608 + (0.7978845608 * 0.044715) * (t * t)))


def pair_weight(block, blank, count):
    return jnp.concatenate(
        [
            jnp.concatenate([block(k, b) if k < 3 else blank, block(k - 1, b) if k > 0 else blank], axis=1)
            for k in range(4)
            for b in range(count)
        ],
        axis=0,
    )


def spatial_weight(weight_ref, layer):
    blank = jnp.zeros(weight_ref.shape[-2:], weight_ref.dtype)
    return pair_weight(lambda k, b: weight_ref[layer, k, b], blank, 3)


def put_shifted(dst, row, cells):
    groups, width, chans = cells.shape
    for shift, moved in ((0, pltpu.roll(cells, 1, 1)), (1, cells), (2, pltpu.roll(cells, width - 1, 1))):
        dst[shift, row] = moved.reshape(groups * width, chans).astype(dst.dtype)


def clear_borders(buf):
    for shift in range(3):
        for row in (0, buf.shape[1] - 1):
            buf[shift, row] = jnp.zeros(buf.shape[2:], buf.dtype)


def edge_tile(cells):
    first, last = cells[:, :TILE], cells[:, cells.shape[1] - TILE :]
    place = lax.broadcasted_iota(jnp.int32, first.shape, 1)
    return pltpu.roll(jnp.where(place < EDGE, first, last), EDGE, 1)


def pack_kernel(side_ref, field_hbm, near_ref, far_ref, tiles, sems):
    cols = field_hbm.shape[2]
    copies = [
        pltpu.make_async_copy(field_hbm.at[:, :, pl.ds(start, TILE)], tiles.at[i], sems.at[i])
        for i, start in enumerate((0, cols - TILE))
    ]
    for copy in copies:
        copy.start()
    for copy in copies:
        copy.wait()
    first = side_ref[0] == 0
    for view in range(tiles.shape[1]):
        head = tiles[0, view].astype(jnp.float32)[:, :EDGE]
        tail = tiles[1, view].astype(jnp.float32)[:, TILE - EDGE :]
        near_ref[view] = jnp.where(first, tail, head).astype(near_ref.dtype)
        far_ref[view] = jnp.where(first, head, tail).astype(far_ref.dtype)


def inner_kernel(field_ref, weight_ref, offset_ref, out_ref, saved_ref, even, odd):
    views, rows, cols, chans = field_ref.shape
    layers = weight_ref.shape[0]
    bufs = (even, odd)
    for buf in bufs:
        clear_borders(buf)
    for row in range(rows):
        cells = field_ref[:, row].astype(jnp.float32)
        put_shifted(even, row + 1, cells)
        saved_ref[0, row] = edge_tile(cells).reshape(views * TILE, chans).astype(saved_ref.dtype)
    for layer in range(layers):
        src, dst = bufs[layer % 2], bufs[(layer + 1) % 2]
        weight = spatial_weight(weight_ref, layer)
        offset = offset_ref[layer]
        for pair in range(rows // 2):
            stacked = jnp.concatenate([src[b, 2 * pair + k] for k in range(4) for b in range(3)], axis=1)
            total = jnp.dot(stacked, weight, preferred_element_type=jnp.float32)
            for r in range(2):
                value = gelu(total[:, r * chans : (r + 1) * chans] + offset)
                row = 2 * pair + r
                if layer == layers - 1:
                    out_ref[row] = value.astype(out_ref.dtype)
                else:
                    cells = value.reshape(views, cols, chans)
                    put_shifted(dst, row + 1, cells)
                    saved_ref[layer + 1, row] = (
                        edge_tile(cells).reshape(views * TILE, chans).astype(saved_ref.dtype)
                    )


def outer_kernel(side_ref, near_ref, far_ref, saved_ref, inner_ref, weight_ref, offset_ref, out_ref, even, odd):
    all_views, rows, _, chans = near_ref.shape
    layers = weight_ref.shape[0]
    cols = inner_ref.shape[1] // all_views
    bufs = (even, odd)
    groups = even.shape[0]
    views = all_views // groups
    first = side_ref[0] == 0
    place = lax.broadcasted_iota(jnp.int32, (views, TILE, chans), 1)

    def kept(layer, row, group):
        part = saved_ref[layer, row, group * views * TILE : (group + 1) * views * TILE]
        return part.astype(jnp.float32).reshape(views, TILE, chans)

    for group in range(groups):
        for buf in bufs:
            clear_borders(buf.at[group])
        span = slice(group * views, (group + 1) * views)
        for row in range(rows):
            near = near_ref[span, row].astype(jnp.float32)
            far = far_ref[span, row].astype(jnp.float32)
            right = jnp.where(first, near, far)
            left = jnp.where(first, far, near)
            own = kept(0, row, group)
            cells = jnp.concatenate([left, own[:, EDGE:], own[:, :EDGE], right], axis=1)
            put_shifted(even.at[group], row + 1, cells)
    for layer in range(layers):
        weight = spatial_weight(weight_ref, layer)
        offset = offset_ref[layer]
        for group in range(groups):
            src, dst = bufs[layer % 2].at[group], bufs[(layer + 1) % 2].at[group]
            stacked = jnp.concatenate(
                [
                    jnp.concatenate([src[b, 2 * pair + k] for pair in range(rows // 2)], axis=0)
                    for k in range(4)
                    for b in range(3)
                ],
                axis=1,
            )
            total = jnp.dot(stacked, weight, preferred_element_type=jnp.float32)
            span = views * 2 * TILE
            for row in range(rows):
                part = total[(row // 2) * span : (row // 2 + 1) * span, (row % 2) * chans : (row % 2 + 1) * chans]
                value = gelu(part + offset).reshape(views, 2 * TILE, chans)
                lower, upper = value[:, :TILE], value[:, TILE:]
                if layer == layers - 1:
                    part = slice(group * views * cols, (group + 1) * views * cols)
                    cells = inner_ref[row, part].astype(jnp.float32).reshape(views, cols, chans)
                    fresh = layers
                    lower = jnp.where(place < fresh, pltpu.roll(lower, EDGE, 1), cells[:, :TILE])
                    upper = jnp.where(place >= TILE - fresh, pltpu.roll(upper, EDGE, 1), cells[:, cols - TILE :])
                    cells = jnp.concatenate([lower, cells[:, TILE : cols - TILE], upper], axis=1)
                    out_ref[row, part] = cells.reshape(views * cols, chans).astype(out_ref.dtype)
                else:
                    own = kept(layer + 1, row, group)
                    lower = jnp.where(place > EDGE + layer, own, lower)
                    upper = jnp.where(place < EDGE - 1 - layer, own, upper)
                    put_shifted(dst, row + 1, jnp.concatenate([lower, upper], axis=1))


def view_pair(sources, pair, views, cols, chans, blank):
    stacked, weight = [], []
    for ref, taps in sources:
        for k in range(4):
            view = 2 * pair + k - 1
            if 0 <= view < views:
                stacked.append(ref[:, view * cols : (view + 1) * cols].reshape(-1, chans))
                weight.append(
                    jnp.concatenate([taps(k) if k < 3 else blank, taps(k - 1) if k > 0 else blank], axis=1)
                )
    return jnp.dot(
        jnp.concatenate(stacked, axis=1), jnp.concatenate(weight, axis=0), preferred_element_type=jnp.float32
    )


def partial_kernel(side_ref, hidden_ref, near_ref, weight_ref, offset_ref, out_ref):
    pairs, _, wide = out_ref.shape
    chans = wide // 2
    views = 2 * pairs
    cols = hidden_ref.shape[1] // views
    near_tap = jnp.where(side_ref[0] == 0, 2, 0)
    blank = jnp.zeros((chans, chans), weight_ref.dtype)
    offset = jnp.concatenate([offset_ref[...]] * 2, axis=1)
    sources = ((hidden_ref, lambda k: weight_ref[1, k]), (near_ref, lambda k: weight_ref[near_tap, k]))
    for pair in range(pairs):
        out_ref[pair] = view_pair(sources, pair, views, cols, chans, blank) + offset


def final_kernel(side_ref, far_ref, partial_ref, weight_ref, field_ref, out_hbm, out, sems):
    views, rows, cols, chans = field_ref.shape
    far_tap = jnp.where(side_ref[0] == 0, 0, 2)
    blank = jnp.zeros((chans, chans), weight_ref.dtype)
    sources = ((far_ref, lambda k: weight_ref[far_tap, k]),)
    copies = []
    for pair in range(views // 2):
        total = view_pair(sources, pair, views, cols, chans, blank) + partial_ref[pair]
        for r in range(2):
            view = 2 * pair + r
            angular = total[:, r * chans : (r + 1) * chans].astype(jnp.bfloat16)
            field = field_ref[view].reshape(rows * cols, chans).astype(jnp.float32)
            out[view] = (field + angular.astype(jnp.float32)).astype(out.dtype).reshape(rows, cols, chans)
        part = pl.ds(2 * pair, 2)
        copies.append(pltpu.make_async_copy(out.at[part], out_hbm.at[part], sems.at[pair]))
        copies[-1].start()
    for copy in copies:
        copy.wait()


def swap(cells, axis, start, count, closed):
    pairs = []
    for i in range(start, count, 2):
        j = i + 1
        if j < count or closed:
            pairs += [(i, j % count), (j % count, i)]
    return lax.ppermute(cells, axis, pairs)


def params(mebibytes):
    return pltpu.CompilerParams(vmem_limit_bytes=mebibytes * 2**20)


def local(light_field, spatial_weights, spatial_offsets, angular_weight, angular_offset):
    views, rows, cols, chans = light_field.shape
    lon_count, view_count = lax.axis_size("lon"), lax.axis_size("view")
    lon_side = lax.rem(lax.axis_index("lon"), 2)[None]
    view_side = lax.rem(lax.axis_index("view"), 2)[None]
    offsets = spatial_offsets[:, None]
    layers = spatial_weights.shape[0]
    half = jnp.bfloat16

    edge = jax.ShapeDtypeStruct((views, rows, EDGE, chans), half)
    near, far = pl.pallas_call(
        pack_kernel,
        out_shape=(edge, edge),
        in_specs=[SMEM, HBM],
        out_specs=(VMEM, VMEM),
        scratch_shapes=[
            pltpu.VMEM((2, views, rows, TILE, chans), half),
            pltpu.SemaphoreType.DMA((2,)),
        ],
        compiler_params=params(4),
        name="pack",
    )(lon_side, pltpu.with_memory_space_constraint(light_field, pltpu.HBM))
    far = swap(far, "lon", 1, lon_count, True)
    near = swap(near, "lon", 0, lon_count, True)

    inner, saved = pl.pallas_call(
        inner_kernel,
        out_shape=(
            jax.ShapeDtypeStruct((rows, views * cols, chans), half),
            jax.ShapeDtypeStruct((layers, rows, views * TILE, chans), half),
        ),
        in_specs=[VMEM] * 3,
        out_specs=(VMEM, VMEM),
        scratch_shapes=[pltpu.VMEM((3, rows + 2, views * cols, chans), half)] * 2,
        compiler_params=params(20),
        name="inner",
    )(light_field, spatial_weights, offsets)
    hidden = pl.pallas_call(
        outer_kernel,
        out_shape=jax.ShapeDtypeStruct((rows, views * cols, chans), half),
        in_specs=[SMEM] + [VMEM] * 6,
        out_specs=VMEM,
        scratch_shapes=[pltpu.VMEM((GROUPS, 3, rows + 2, views // GROUPS * 2 * TILE, chans), half)] * 2,
        compiler_params=params(16),
        name="outer",
    )(lon_side, near, far, saved, inner, spatial_weights, offsets)

    far_rows = swap(hidden, "view", 1, view_count, False)
    near_rows = swap(hidden, "view", 0, view_count, False)
    partial = pl.pallas_call(
        partial_kernel,
        out_shape=jax.ShapeDtypeStruct((views // 2, rows * cols, 2 * chans), jnp.float32),
        in_specs=[SMEM] + [VMEM] * 4,
        out_specs=VMEM,
        compiler_params=params(8),
        name="partial",
    )(view_side, hidden, near_rows, angular_weight, angular_offset[None])
    return pl.pallas_call(
        final_kernel,
        out_shape=jax.ShapeDtypeStruct(light_field.shape, half),
        in_specs=[SMEM] + [VMEM] * 4,
        out_specs=HBM,
        scratch_shapes=[
            pltpu.VMEM(light_field.shape, half),
            pltpu.SemaphoreType.DMA((views // 2,)),
        ],
        compiler_params=params(8),
        name="final",
    )(view_side, far_rows, partial, angular_weight, light_field)


def solution(mesh):
    return jax.shard_map(
        local,
        mesh=mesh,
        in_specs=(P(("grp", "view"), None, "lon", None), P(), P(), P(), P()),
        out_specs=P(("grp", "view"), None, "lon", None),
        check_vma=False,
    )
```

```python
import jax
import jax.numpy as jnp
from jax import lax
from jax.experimental import pallas as pl
from jax.experimental.pallas import tpu as pltpu
from jax.sharding import PartitionSpec as P


EDGE = 4
TILE = 8
GROUPS = 4
VMEM = pl.BlockSpec(memory_space=pltpu.VMEM)
SMEM = pl.BlockSpec(memory_space=pltpu.SMEM)
HBM = pl.BlockSpec(memory_space=pl.ANY)


def gelu(t):
    half = 0.5 * t
    return half + half * jnp.tanh(t * (0.7978845608 + (0.7978845608 * 0.044715) * (t * t)))


def pair_weight(block, blank, count):
    return jnp.concatenate(
        [
            jnp.concatenate([block(k, b) if k < 3 else blank, block(k - 1, b) if k > 0 else blank], axis=1)
            for k in range(4)
            for b in range(count)
        ],
        axis=0,
    )


def spatial_weight(weight_ref, layer):
    blank = jnp.zeros(weight_ref.shape[-2:], weight_ref.dtype)
    return pair_weight(lambda k, b: weight_ref[layer, k, b], blank, 3)


def put_shifted(dst, row, cells):
    groups, width, chans = cells.shape
    for shift, moved in ((0, pltpu.roll(cells, 1, 1)), (1, cells), (2, pltpu.roll(cells, width - 1, 1))):
        dst[shift, row] = moved.reshape(groups * width, chans).astype(dst.dtype)


def clear_borders(buf):
    for shift in range(3):
        for row in (0, buf.shape[1] - 1):
            buf[shift, row] = jnp.zeros(buf.shape[2:], buf.dtype)


def pack_kernel(
    side_ref, lead_ref, field_hbm, weight_hbm, spatial_hbm, angular_hbm,
    near_ref, far_ref, spatial_ref, angular_ref, mid_ref, edge_ref, saved_ref,
    tiles, field, weight, even, odd, sems,
):
    cols = field_hbm.shape[2]
    copies = [
        pltpu.make_async_copy(field_hbm.at[:, :, pl.ds(start, TILE)], tiles.at[i], sems.at[i])
        for i, start in enumerate((0, cols - TILE))
    ]
    copies.append(pltpu.make_async_copy(spatial_hbm, spatial_ref, sems.at[2]))
    copies.append(pltpu.make_async_copy(angular_hbm, angular_ref, sems.at[3]))
    for copy in copies:
        copy.start()
    for copy in copies:
        copy.wait()
    first = side_ref[0] == 0
    for view in range(tiles.shape[1]):
        head = tiles[0, view].astype(jnp.float32)[:, :EDGE]
        tail = tiles[1, view].astype(jnp.float32)[:, TILE - EDGE :]
        near_ref[view] = jnp.where(first, tail, head).astype(near_ref.dtype)
        far_ref[view] = jnp.where(first, head, tail).astype(far_ref.dtype)

    @pl.when(lead_ref[0] == 0)
    def _():
        loads = (
            pltpu.make_async_copy(field_hbm, field, sems.at[0]),
            pltpu.make_async_copy(weight_hbm, weight, sems.at[1]),
        )
        for load in loads:
            load.start()
        for load in loads:
            load.wait()
        inner_layers(field, weight, spatial_ref, mid_ref, edge_ref, saved_ref, even, odd)


def inner_kernel(
    lead_ref, field_ref, weight_ref, offset_ref, mid_in, edge_in, saved_in,
    mid_ref, edge_ref, saved_ref, even, odd,
):
    @pl.when(lead_ref[0] == 0)
    def _():
        mid_ref[...] = mid_in[...]
        edge_ref[...] = edge_in[...]
        saved_ref[...] = saved_in[...]

    @pl.when(lead_ref[0] != 0)
    def _():
        inner_layers(field_ref, weight_ref, offset_ref, mid_ref, edge_ref, saved_ref, even, odd)


def inner_layers(field_ref, weight_ref, offset_ref, mid_ref, edge_ref, saved_ref, even, odd):
    views, rows, cols, chans = field_ref.shape
    layers = weight_ref.shape[0]
    mid = cols - TILE
    bufs = (even, odd)
    for buf in bufs:
        clear_borders(buf)

    def keep(layer, row, cells):
        saved_ref[layer, row] = cells[:, mid:].reshape(views * TILE, chans).astype(saved_ref.dtype)

    for row in range(rows):
        cells = pltpu.roll(field_ref[:, row].astype(jnp.float32), cols - EDGE, 1)
        put_shifted(even, row + 1, cells)
        keep(0, row, cells)
    for layer in range(layers):
        src, dst = bufs[layer % 2], bufs[(layer + 1) % 2]
        weight = spatial_weight(weight_ref, layer)
        offset = offset_ref[layer : layer + 1]
        for pair in range(rows // 2):
            stacked = jnp.concatenate([src[b, 2 * pair + k] for k in range(4) for b in range(3)], axis=1)
            total = jnp.dot(stacked, weight, preferred_element_type=jnp.float32)
            cells = [
                gelu(total[:, r * chans : (r + 1) * chans] + offset).reshape(views, cols, chans) for r in range(2)
            ]
            if layer == layers - 1:
                part = pl.ds(2 * mid * pair, 2 * mid)
                mid_ref[:, part] = jnp.concatenate([c[:, :mid] for c in cells], axis=1).astype(mid_ref.dtype)
                part = pl.ds(2 * TILE * pair, 2 * TILE)
                edge_ref[:, part] = jnp.concatenate([c[:, mid:] for c in cells], axis=1).astype(edge_ref.dtype)
            else:
                for r in range(2):
                    put_shifted(dst, 2 * pair + r + 1, cells[r])
                    keep(layer + 1, 2 * pair + r, cells[r])


def outer_kernel(
    side_ref, near_ref, far_ref, saved_ref, mid_ref, inner_ref, weight_ref, offset_ref,
    whole_ref, edge_ref, even, odd,
):
    all_views, rows, _, chans = near_ref.shape
    layers = weight_ref.shape[0]
    bufs = (even, odd)
    groups = even.shape[0]
    views = all_views // groups
    mid = mid_ref.shape[1]
    first = side_ref[0] == 0
    place = lax.broadcasted_iota(jnp.int32, (views, TILE, chans), 1)
    whole_ref[:, :mid] = mid_ref[...]

    def kept(layer, row, group):
        part = saved_ref[layer, row, group * views * TILE : (group + 1) * views * TILE]
        return part.astype(jnp.float32).reshape(views, TILE, chans)

    for group in range(groups):
        for buf in bufs:
            clear_borders(buf.at[group])
        span = slice(group * views, (group + 1) * views)
        for row in range(rows):
            near = near_ref[span, row].astype(jnp.float32)
            far = far_ref[span, row].astype(jnp.float32)
            right = jnp.where(first, near, far)
            left = jnp.where(first, far, near)
            own = kept(0, row, group)
            cells = jnp.concatenate([left, own[:, EDGE:], own[:, :EDGE], right], axis=1)
            put_shifted(even.at[group], row + 1, cells)
    for layer in range(layers):
        weight = spatial_weight(weight_ref, layer)
        offset = offset_ref[layer : layer + 1]
        fresh = layer + 1
        for group in range(groups):
            src, dst = bufs[layer % 2].at[group], bufs[(layer + 1) % 2].at[group]
            stacked = jnp.concatenate(
                [
                    jnp.concatenate([src[b, 2 * pair + k] for pair in range(rows // 2)], axis=0)
                    for k in range(4)
                    for b in range(3)
                ],
                axis=1,
            )
            total = jnp.dot(stacked, weight, preferred_element_type=jnp.float32)
            span = views * 2 * TILE
            part = slice(group * views, (group + 1) * views)
            for pair in range(rows // 2):
                ends = []
                for r in range(2):
                    value = gelu(
                        total[pair * span : (pair + 1) * span, r * chans : (r + 1) * chans] + offset
                    ).reshape(views, 2 * TILE, chans)
                    lower, upper = value[:, :TILE], value[:, TILE:]
                    row = 2 * pair + r
                    if layer == layers - 1:
                        ends.append((lower, upper))
                    else:
                        own = kept(fresh, row, group)
                        lower = jnp.where(place >= EDGE + fresh, own, lower)
                        upper = jnp.where(place < EDGE - fresh, own, upper)
                        put_shifted(dst, row + 1, jnp.concatenate([lower, upper], axis=1))
                if ends:
                    own = inner_ref[part, 2 * TILE * pair : 2 * TILE * (pair + 1)].astype(jnp.float32)
                    done = []
                    for r, (lower, upper) in enumerate(ends):
                        tile = own[:, r * TILE : (r + 1) * TILE]
                        tile = jnp.where((place >= EDGE) & (place < EDGE + fresh), lower, tile)
                        done.append(jnp.where((place < EDGE) & (place >= EDGE - fresh), upper, tile))
                    done = jnp.concatenate(done, axis=1).astype(edge_ref.dtype)
                    edge_ref[part, 2 * TILE * pair : 2 * TILE * (pair + 1)] = done
                    whole_ref[part, mid + 2 * TILE * pair : mid + 2 * TILE * (pair + 1)] = done


def view_pair(sources, pair, views, blank):
    stacked, weight = [], []
    for load, taps in sources:
        for k in range(4):
            view = 2 * pair + k - 1
            if 0 <= view < views:
                stacked.append(load(view))
                weight.append(
                    jnp.concatenate([taps(k) if k < 3 else blank, taps(k - 1) if k > 0 else blank], axis=1)
                )
    return jnp.dot(
        jnp.concatenate(stacked, axis=1), jnp.concatenate(weight, axis=0), preferred_element_type=jnp.float32
    )


def partial_kernel(side_ref, hidden_ref, near_ref, weight_ref, offset_ref, out_ref):
    pairs, _, wide = out_ref.shape
    chans = wide // 2
    near_tap = jnp.where(side_ref[0] == 0, 2, 0)
    blank = jnp.zeros((chans, chans), weight_ref.dtype)
    offset = jnp.concatenate([offset_ref[...]] * 2, axis=1)
    sources = (
        (lambda view: hidden_ref[view], lambda k: weight_ref[1, k]),
        (lambda view: near_ref[view], lambda k: weight_ref[near_tap, k]),
    )
    for pair in range(pairs):
        out_ref[pair] = view_pair(sources, pair, 2 * pairs, blank) + offset


def final_kernel(side_ref, mid_ref, edge_ref, partial_ref, weight_ref, field_ref, out_hbm, out, sems):
    views, rows, cols, chans = field_ref.shape
    far_tap = jnp.where(side_ref[0] == 0, 0, 2)
    blank = jnp.zeros((chans, chans), weight_ref.dtype)
    mid = rows * (cols - TILE)
    sources = (
        (lambda view: jnp.concatenate([mid_ref[view], edge_ref[view]], axis=0), lambda k: weight_ref[far_tap, k]),
    )
    copies = []
    for pair in range(views // 2):
        total = view_pair(sources, pair, views, blank) + partial_ref[pair]
        for r in range(2):
            view = 2 * pair + r
            angular = total[:, r * chans : (r + 1) * chans].astype(jnp.bfloat16).astype(jnp.float32)
            cells = jnp.concatenate(
                [angular[:mid].reshape(rows, cols - TILE, chans), angular[mid:].reshape(rows, TILE, chans)], axis=1
            )
            out[view] = (field_ref[view].astype(jnp.float32) + pltpu.roll(cells, EDGE, 1)).astype(out.dtype)
        part = pl.ds(2 * pair, 2)
        copies.append(pltpu.make_async_copy(out.at[part], out_hbm.at[part], sems.at[pair]))
        copies[-1].start()
    for copy in copies:
        copy.wait()


def swap(cells, axis, start, count, closed):
    pairs = []
    for i in range(start, count, 2):
        j = i + 1
        if j < count or closed:
            pairs += [(i, j % count), (j % count, i)]
    return lax.ppermute(cells, axis, pairs)


def params(mebibytes):
    return pltpu.CompilerParams(vmem_limit_bytes=mebibytes * 2**20)


def local(light_field, spatial_weights, spatial_offsets, angular_weight, angular_offset):
    views, rows, cols, chans = light_field.shape
    lon_count, view_count = lax.axis_size("lon"), lax.axis_size("view")
    lead = lax.axis_index("lon")[None]
    lon_side = lax.rem(lax.axis_index("lon"), 2)[None]
    view_side = lax.rem(lax.axis_index("view"), 2)[None]
    layers = spatial_weights.shape[0]
    half = jnp.bfloat16

    def shaped(*shape):
        return jax.ShapeDtypeStruct(shape, half)

    edges = shaped(views, rows, EDGE, chans)
    inner_shapes = (
        shaped(views, rows * (cols - TILE), chans),
        shaped(views, rows * TILE, chans),
        shaped(layers, rows, views * TILE, chans),
    )
    biases = [jax.ShapeDtypeStruct(b.shape, jnp.float32) for b in (spatial_offsets, angular_offset[None])]
    inner_scratch = [pltpu.VMEM((3, rows + 2, views * cols, chans), half)] * 2
    in_hbm = lambda array: pltpu.with_memory_space_constraint(array, pltpu.HBM)
    near, far, spatial_bias, angular_bias, *early = pl.pallas_call(
        pack_kernel,
        out_shape=(edges, edges, *biases, *inner_shapes),
        in_specs=[SMEM, SMEM, HBM, HBM, HBM, HBM],
        out_specs=(VMEM,) * 7,
        scratch_shapes=[
            pltpu.VMEM((2, views, rows, TILE, chans), half),
            pltpu.VMEM(light_field.shape, half),
            pltpu.VMEM(spatial_weights.shape, half),
            *inner_scratch,
            pltpu.SemaphoreType.DMA((4,)),
        ],
        compiler_params=params(20),
        cost_estimate=pl.CostEstimate(flops=2 * 10**9, bytes_accessed=10**7, transcendentals=0),
        name="pack",
    )(lon_side, lead, in_hbm(light_field), in_hbm(spatial_weights), in_hbm(spatial_offsets), in_hbm(angular_offset[None]))
    far = swap(far, "lon", 1, lon_count, True)
    near = swap(near, "lon", 0, lon_count, True)

    mid, edge, saved = pl.pallas_call(
        inner_kernel,
        out_shape=inner_shapes,
        in_specs=[SMEM] + [VMEM] * 6,
        out_specs=(VMEM,) * 3,
        scratch_shapes=inner_scratch,
        compiler_params=params(20),
        name="inner",
    )(lead, light_field, spatial_weights, spatial_bias, *early)
    far_mid = swap(mid, "view", 1, view_count, False)
    whole, edge = pl.pallas_call(
        outer_kernel,
        out_shape=(shaped(views, rows * cols, chans), inner_shapes[1]),
        in_specs=[SMEM] + [VMEM] * 7,
        out_specs=(VMEM, VMEM),
        scratch_shapes=[pltpu.VMEM((GROUPS, 3, rows + 2, views // GROUPS * 2 * TILE, chans), half)] * 2,
        compiler_params=params(16),
        name="outer",
    )(lon_side, near, far, saved, mid, edge, spatial_weights, spatial_bias)
    far_edge = swap(edge, "view", 1, view_count, False)
    near_rows = swap(whole, "view", 0, view_count, False)
    partial = pl.pallas_call(
        partial_kernel,
        out_shape=jax.ShapeDtypeStruct((views // 2, rows * cols, 2 * chans), jnp.float32),
        in_specs=[SMEM] + [VMEM] * 4,
        out_specs=VMEM,
        compiler_params=params(8),
        name="partial",
    )(view_side, whole, near_rows, angular_weight, angular_bias)
    return pl.pallas_call(
        final_kernel,
        out_shape=jax.ShapeDtypeStruct(light_field.shape, half),
        in_specs=[SMEM] + [VMEM] * 5,
        out_specs=HBM,
        scratch_shapes=[
            pltpu.VMEM(light_field.shape, half),
            pltpu.SemaphoreType.DMA((views // 2,)),
        ],
        compiler_params=params(8),
        name="final",
    )(view_side, far_mid, far_edge, partial, angular_weight, light_field)


def solution(mesh):
    return jax.shard_map(
        local,
        mesh=mesh,
        in_specs=(P(("grp", "view"), None, "lon", None), P(), P(), P(), P()),
        out_specs=P(("grp", "view"), None, "lon", None),
        check_vma=False,
    )
```

```python
import jax
import jax.numpy as jnp
from jax import lax
from jax.experimental import pallas as pl
from jax.experimental.pallas import tpu as pltpu
from jax.sharding import PartitionSpec as P


EDGE = 4
TILE = 8
GROUPS = 4
VMEM = pl.BlockSpec(memory_space=pltpu.VMEM)
SMEM = pl.BlockSpec(memory_space=pltpu.SMEM)
HBM = pl.BlockSpec(memory_space=pl.ANY)


def gelu(t):
    half = 0.5 * t
    return half + half * jnp.tanh(t * (0.7978845608 + (0.7978845608 * 0.044715) * (t * t)))


def pair_weight(block, blank, count):
    return jnp.concatenate(
        [
            jnp.concatenate([block(k, b) if k < 3 else blank, block(k - 1, b) if k > 0 else blank], axis=1)
            for k in range(4)
            for b in range(count)
        ],
        axis=0,
    )


def spatial_weight(weight_ref, layer):
    blank = jnp.zeros(weight_ref.shape[-2:], weight_ref.dtype)
    return pair_weight(lambda k, b: weight_ref[layer, k, b], blank, 3)


def put_shifted(dst, row, cells):
    groups, width, chans = cells.shape
    for shift, moved in ((0, pltpu.roll(cells, 1, 1)), (1, cells), (2, pltpu.roll(cells, width - 1, 1))):
        dst[shift, row] = moved.reshape(groups * width, chans).astype(dst.dtype)


def clear_borders(buf):
    for shift in range(3):
        for row in (0, buf.shape[1] - 1):
            buf[shift, row] = jnp.zeros(buf.shape[2:], buf.dtype)


def pack_kernel(
    side_ref, lead_ref, field_hbm, weight_hbm, spatial_hbm, angular_hbm,
    near_ref, far_ref, spatial_ref, angular_ref, mid_ref, edge_ref, saved_ref,
    tiles, field, weight, even, odd, sems,
):
    cols = field_hbm.shape[2]
    copies = [
        pltpu.make_async_copy(field_hbm.at[:, :, pl.ds(start, TILE)], tiles.at[i], sems.at[i])
        for i, start in enumerate((0, cols - TILE))
    ]
    copies.append(pltpu.make_async_copy(spatial_hbm, spatial_ref, sems.at[2]))
    copies.append(pltpu.make_async_copy(angular_hbm, angular_ref, sems.at[3]))
    for copy in copies:
        copy.start()
    for copy in copies:
        copy.wait()
    first = side_ref[0] == 0
    for view in range(tiles.shape[1]):
        head = tiles[0, view].astype(jnp.float32)[:, :EDGE]
        tail = tiles[1, view].astype(jnp.float32)[:, TILE - EDGE :]
        near_ref[view] = jnp.where(first, tail, head).astype(near_ref.dtype)
        far_ref[view] = jnp.where(first, head, tail).astype(far_ref.dtype)

    @pl.when(lead_ref[0] != 0)
    def _():
        loads = (
            pltpu.make_async_copy(field_hbm, field, sems.at[0]),
            pltpu.make_async_copy(weight_hbm, weight, sems.at[1]),
        )
        for load in loads:
            load.start()
        for load in loads:
            load.wait()
        inner_layers(field, weight, spatial_ref, mid_ref, edge_ref, saved_ref, even, odd)


def inner_kernel(
    lead_ref, field_ref, weight_ref, offset_ref, mid_in, edge_in, saved_in,
    mid_ref, edge_ref, saved_ref, even, odd,
):
    @pl.when(lead_ref[0] != 0)
    def _():
        mid_ref[...] = mid_in[...]
        edge_ref[...] = edge_in[...]
        saved_ref[...] = saved_in[...]

    @pl.when(lead_ref[0] == 0)
    def _():
        inner_layers(field_ref, weight_ref, offset_ref, mid_ref, edge_ref, saved_ref, even, odd)


def inner_layers(field_ref, weight_ref, offset_ref, mid_ref, edge_ref, saved_ref, even, odd):
    views, rows, cols, chans = field_ref.shape
    layers = weight_ref.shape[0]
    mid = cols - TILE
    bufs = (even, odd)
    for buf in bufs:
        clear_borders(buf)

    def keep(layer, row, cells):
        saved_ref[layer, row] = cells[:, mid:].reshape(views * TILE, chans).astype(saved_ref.dtype)

    for row in range(rows):
        cells = pltpu.roll(field_ref[:, row].astype(jnp.float32), cols - EDGE, 1)
        put_shifted(even, row + 1, cells)
        keep(0, row, cells)
    for layer in range(layers):
        src, dst = bufs[layer % 2], bufs[(layer + 1) % 2]
        weight = spatial_weight(weight_ref, layer)
        offset = offset_ref[layer : layer + 1]
        for pair in range(rows // 2):
            stacked = jnp.concatenate([src[b, 2 * pair + k] for k in range(4) for b in range(3)], axis=1)
            total = jnp.dot(stacked, weight, preferred_element_type=jnp.float32)
            cells = [
                gelu(total[:, r * chans : (r + 1) * chans] + offset).reshape(views, cols, chans) for r in range(2)
            ]
            if layer == layers - 1:
                part = pl.ds(2 * mid * pair, 2 * mid)
                mid_ref[:, part] = jnp.concatenate([c[:, :mid] for c in cells], axis=1).astype(mid_ref.dtype)
                part = pl.ds(2 * TILE * pair, 2 * TILE)
                edge_ref[:, part] = jnp.concatenate([c[:, mid:] for c in cells], axis=1).astype(edge_ref.dtype)
            else:
                for r in range(2):
                    put_shifted(dst, 2 * pair + r + 1, cells[r])
                    keep(layer + 1, 2 * pair + r, cells[r])


def outer_kernel(
    side_ref, near_ref, rest_ref, far_ref, saved_ref, mid_ref, inner_ref, weight_ref, offset_ref,
    whole_ref, edge_ref, even, odd,
):
    all_views, rows, _, chans = near_ref.shape
    layers = weight_ref.shape[0]
    bufs = (even, odd)
    groups = even.shape[0]
    views = all_views // groups
    mid = mid_ref.shape[1]
    first = side_ref[0] == 0
    place = lax.broadcasted_iota(jnp.int32, (views, TILE, chans), 1)
    whole_ref[:, :mid] = mid_ref[...]

    def kept(layer, row, group):
        part = saved_ref[layer, row, group * views * TILE : (group + 1) * views * TILE]
        return part.astype(jnp.float32).reshape(views, TILE, chans)

    for group in range(groups):
        for buf in bufs:
            clear_borders(buf.at[group])
        span = slice(group * views, (group + 1) * views)
        for row in range(rows):
            near = near_ref[span, row].astype(jnp.float32) + rest_ref[span, row].astype(jnp.float32)
            far = far_ref[span, row].astype(jnp.float32)
            right = jnp.where(first, near, far)
            left = jnp.where(first, far, near)
            own = kept(0, row, group)
            cells = jnp.concatenate([left, own[:, EDGE:], own[:, :EDGE], right], axis=1)
            put_shifted(even.at[group], row + 1, cells)
    for layer in range(layers):
        weight = spatial_weight(weight_ref, layer)
        offset = offset_ref[layer : layer + 1]
        fresh = layer + 1
        for group in range(groups):
            src, dst = bufs[layer % 2].at[group], bufs[(layer + 1) % 2].at[group]
            stacked = jnp.concatenate(
                [
                    jnp.concatenate([src[b, 2 * pair + k] for pair in range(rows // 2)], axis=0)
                    for k in range(4)
                    for b in range(3)
                ],
                axis=1,
            )
            total = jnp.dot(stacked, weight, preferred_element_type=jnp.float32)
            span = views * 2 * TILE
            part = slice(group * views, (group + 1) * views)
            for pair in range(rows // 2):
                ends = []
                for r in range(2):
                    value = gelu(
                        total[pair * span : (pair + 1) * span, r * chans : (r + 1) * chans] + offset
                    ).reshape(views, 2 * TILE, chans)
                    lower, upper = value[:, :TILE], value[:, TILE:]
                    row = 2 * pair + r
                    if layer == layers - 1:
                        ends.append((lower, upper))
                    else:
                        own = kept(fresh, row, group)
                        lower = jnp.where(place >= EDGE + fresh, own, lower)
                        upper = jnp.where(place < EDGE - fresh, own, upper)
                        put_shifted(dst, row + 1, jnp.concatenate([lower, upper], axis=1))
                if ends:
                    own = inner_ref[part, 2 * TILE * pair : 2 * TILE * (pair + 1)].astype(jnp.float32)
                    done = []
                    for r, (lower, upper) in enumerate(ends):
                        tile = own[:, r * TILE : (r + 1) * TILE]
                        tile = jnp.where((place >= EDGE) & (place < EDGE + fresh), lower, tile)
                        done.append(jnp.where((place < EDGE) & (place >= EDGE - fresh), upper, tile))
                    done = jnp.concatenate(done, axis=1).astype(edge_ref.dtype)
                    edge_ref[part, 2 * TILE * pair : 2 * TILE * (pair + 1)] = done
                    whole_ref[part, mid + 2 * TILE * pair : mid + 2 * TILE * (pair + 1)] = done


def view_pair(sources, pair, views, blank):
    stacked, weight = [], []
    for load, taps in sources:
        for k in range(4):
            view = 2 * pair + k - 1
            if 0 <= view < views:
                stacked.append(load(view))
                weight.append(
                    jnp.concatenate([taps(k) if k < 3 else blank, taps(k - 1) if k > 0 else blank], axis=1)
                )
    return jnp.dot(
        jnp.concatenate(stacked, axis=1), jnp.concatenate(weight, axis=0), preferred_element_type=jnp.float32
    )


def partial_kernel(side_ref, hidden_ref, lead_ref, rest_ref, edge_ref, weight_ref, offset_ref, out_ref):
    pairs, _, wide = out_ref.shape
    chans = wide // 2
    far_tap = jnp.where(side_ref[0] == 0, 0, 2)
    blank = jnp.zeros((chans, chans), weight_ref.dtype)
    offset = jnp.concatenate([offset_ref[...]] * 2, axis=1)
    sources = (
        (lambda view: hidden_ref[view], lambda k: weight_ref[1, k]),
        (
            lambda view: jnp.concatenate([lead_ref[view] + rest_ref[view], edge_ref[view]], axis=0),
            lambda k: weight_ref[far_tap, k],
        ),
    )
    for pair in range(pairs):
        out_ref[pair] = view_pair(sources, pair, 2 * pairs, blank) + offset


def final_kernel(side_ref, near_ref, partial_ref, weight_ref, field_ref, out_hbm, out, sems):
    views, rows, cols, chans = field_ref.shape
    near_tap = jnp.where(side_ref[0] == 0, 2, 0)
    blank = jnp.zeros((chans, chans), weight_ref.dtype)
    mid = rows * (cols - TILE)
    sources = ((lambda view: near_ref[view], lambda k: weight_ref[near_tap, k]),)
    copies = []
    for pair in range(views // 2):
        total = view_pair(sources, pair, views, blank) + partial_ref[pair]
        for r in range(2):
            view = 2 * pair + r
            angular = total[:, r * chans : (r + 1) * chans].astype(jnp.bfloat16).astype(jnp.float32)
            cells = jnp.concatenate(
                [angular[:mid].reshape(rows, cols - TILE, chans), angular[mid:].reshape(rows, TILE, chans)], axis=1
            )
            out[view] = (field_ref[view].astype(jnp.float32) + pltpu.roll(cells, EDGE, 1)).astype(out.dtype)
        part = pl.ds(2 * pair, 2)
        copies.append(pltpu.make_async_copy(out.at[part], out_hbm.at[part], sems.at[pair]))
        copies[-1].start()
    for copy in copies:
        copy.wait()


def neighbours(starts, count, closed=False):
    pairs = []
    for i in starts:
        if i + 1 < count or closed:
            pairs += [(i, (i + 1) % count), ((i + 1) % count, i)]
    return pairs


def params(mebibytes):
    return pltpu.CompilerParams(vmem_limit_bytes=mebibytes * 2**20)


def local(light_field, spatial_weights, spatial_offsets, angular_weight, angular_offset):
    views, rows, cols, chans = light_field.shape
    lon_count, view_count = lax.axis_size("lon"), lax.axis_size("view")
    lon, view = lax.axis_index("lon"), lax.axis_index("view")
    lead = ((lon == 0) & (view > 0) & (view < view_count - 1)).astype(jnp.int32)[None]
    lon_side, view_side = lax.rem(lon, 2)[None], lax.rem(view, 2)[None]
    layers = spatial_weights.shape[0]
    half = jnp.bfloat16

    def shaped(*shape):
        return jax.ShapeDtypeStruct(shape, half)

    edges = shaped(views, rows, EDGE, chans)
    inner_shapes = (
        shaped(views, rows * (cols - TILE), chans),
        shaped(views, rows * TILE, chans),
        shaped(layers, rows, views * TILE, chans),
    )
    biases = [jax.ShapeDtypeStruct(b.shape, jnp.float32) for b in (spatial_offsets, angular_offset[None])]
    inner_scratch = [pltpu.VMEM((3, rows + 2, views * cols, chans), half)] * 2
    in_hbm = lambda array: pltpu.with_memory_space_constraint(array, pltpu.HBM)
    near, far, spatial_bias, angular_bias, *early = pl.pallas_call(
        pack_kernel,
        out_shape=(edges, edges, *biases, *inner_shapes),
        in_specs=[SMEM, SMEM, HBM, HBM, HBM, HBM],
        out_specs=(VMEM,) * 7,
        scratch_shapes=[
            pltpu.VMEM((2, views, rows, TILE, chans), half),
            pltpu.VMEM(light_field.shape, half),
            pltpu.VMEM(spatial_weights.shape, half),
            *inner_scratch,
            pltpu.SemaphoreType.DMA((4,)),
        ],
        compiler_params=params(12),
        cost_estimate=pl.CostEstimate(flops=2 * 10**9, bytes_accessed=10**7, transcendentals=0),
        name="pack",
    )(lon_side, lead, in_hbm(light_field), in_hbm(spatial_weights), in_hbm(spatial_offsets), in_hbm(angular_offset[None]))
    far_views = neighbours(range(1, view_count, 2), view_count)
    rest_views = [
        (line * view_count + i, line * view_count + j) for line in range(1, lon_count) for i, j in far_views
    ]
    near_lead = lax.ppermute(near, "lon", neighbours(range(0, 2, 2), lon_count))
    mid_lead = lax.ppermute(early[0], ("lon", "view"), far_views)
    far = lax.ppermute(far, "lon", neighbours(range(1, lon_count, 2), lon_count, True))
    near_rest = lax.ppermute(near, "lon", neighbours(range(2, lon_count, 2), lon_count))

    mid, edge, saved = pl.pallas_call(
        inner_kernel,
        out_shape=inner_shapes,
        in_specs=[SMEM] + [VMEM] * 6,
        out_specs=(VMEM,) * 3,
        scratch_shapes=inner_scratch,
        compiler_params=params(12),
        name="inner",
    )(lead, light_field, spatial_weights, spatial_bias, *early)
    mid_rest = lax.ppermute(mid, ("lon", "view"), rest_views)
    whole, edge = pl.pallas_call(
        outer_kernel,
        out_shape=(shaped(views, rows * cols, chans), inner_shapes[1]),
        in_specs=[SMEM] + [VMEM] * 8,
        out_specs=(VMEM, VMEM),
        scratch_shapes=[pltpu.VMEM((GROUPS, 3, rows + 2, views // GROUPS * 2 * TILE, chans), half)] * 2,
        compiler_params=params(6),
        name="outer",
    )(lon_side, near_lead, near_rest, far, saved, mid, edge, spatial_weights, spatial_bias)
    far_edge = lax.ppermute(edge, "view", far_views)
    near_rows = lax.ppermute(whole, "view", neighbours(range(0, view_count, 2), view_count))
    partial = pl.pallas_call(
        partial_kernel,
        out_shape=jax.ShapeDtypeStruct((views // 2, rows * cols, 2 * chans), jnp.float32),
        in_specs=[SMEM] + [VMEM] * 6,
        out_specs=VMEM,
        compiler_params=params(6),
        name="partial",
    )(view_side, whole, mid_lead, mid_rest, far_edge, angular_weight, angular_bias)
    return pl.pallas_call(
        final_kernel,
        out_shape=jax.ShapeDtypeStruct(light_field.shape, half),
        in_specs=[SMEM] + [VMEM] * 4,
        out_specs=HBM,
        scratch_shapes=[
            pltpu.VMEM(light_field.shape, half),
            pltpu.SemaphoreType.DMA((views // 2,)),
        ],
        compiler_params=params(6),
        name="final",
    )(view_side, near_rows, partial, angular_weight, light_field)


def solution(mesh):
    return jax.shard_map(
        local,
        mesh=mesh,
        in_specs=(P(("grp", "view"), None, "lon", None), P(), P(), P(), P()),
        out_specs=P(("grp", "view"), None, "lon", None),
        check_vma=False,
    )
```

```python
import jax
import jax.numpy as jnp
from jax import lax
from jax.experimental import pallas as pl
from jax.experimental.pallas import tpu as pltpu
from jax.sharding import PartitionSpec as P


EDGE = 4
TILE = 8
GROUPS = 2
VMEM = pl.BlockSpec(memory_space=pltpu.VMEM)
SMEM = pl.BlockSpec(memory_space=pltpu.SMEM)
HBM = pl.BlockSpec(memory_space=pl.ANY)


def gelu(t):
    half = 0.5 * t
    return half + half * jnp.tanh(t * (0.7978845608 + (0.7978845608 * 0.044715) * (t * t)))


def pair_weight(block, blank, count):
    return jnp.concatenate(
        [
            jnp.concatenate([block(k, b) if k < 3 else blank, block(k - 1, b) if k > 0 else blank], axis=1)
            for k in range(4)
            for b in range(count)
        ],
        axis=0,
    )


def spatial_weight(weight_ref, layer):
    blank = jnp.zeros(weight_ref.shape[-2:], weight_ref.dtype)
    return pair_weight(lambda k, b: weight_ref[layer, k, b], blank, 3)


def put_shifted(dst, row, cells):
    groups, width, chans = cells.shape
    for shift, moved in ((0, pltpu.roll(cells, 1, 1)), (1, cells), (2, pltpu.roll(cells, width - 1, 1))):
        dst[shift, row] = moved.reshape(groups * width, chans).astype(dst.dtype)


def clear_borders(buf):
    for shift in range(3):
        for row in (0, buf.shape[1] - 1):
            buf[shift, row] = jnp.zeros(buf.shape[2:], buf.dtype)


def pack_kernel(
    side_ref, lead_ref, field_hbm, weight_hbm, spatial_hbm, angular_hbm,
    near_ref, far_ref, spatial_ref, angular_ref, mid_ref, edge_ref, saved_ref,
    tiles, columns, field, weight, even, odd, sems,
):
    cols = field_hbm.shape[2]
    reach, lines, chans = near_ref.shape
    copies = [
        pltpu.make_async_copy(field_hbm.at[:, :, pl.ds(start, TILE)], tiles.at[i], sems.at[i])
        for i, start in enumerate((0, cols - TILE))
    ]
    copies.append(pltpu.make_async_copy(spatial_hbm, spatial_ref, sems.at[2]))
    copies.append(pltpu.make_async_copy(angular_hbm, angular_ref, sems.at[3]))
    for copy in copies:
        copy.start()
    for copy in copies:
        copy.wait()
    first = side_ref[0] == 0
    for i in range(2):
        columns[i] = tiles[i].astype(jnp.float32).reshape(lines * TILE, chans)
    for c in range(reach):
        head = columns[0, pl.ds(c, lines, stride=TILE)]
        tail = columns[1, pl.ds(TILE - reach + c, lines, stride=TILE)]
        near_ref[c] = jnp.where(first, tail, head).astype(near_ref.dtype)
        far_ref[c] = jnp.where(first, head, tail).astype(far_ref.dtype)

    @pl.when(lead_ref[0] != 0)
    def _():
        loads = (
            pltpu.make_async_copy(field_hbm, field, sems.at[0]),
            pltpu.make_async_copy(weight_hbm, weight, sems.at[1]),
        )
        for load in loads:
            load.start()
        for load in loads:
            load.wait()
        inner_layers(field, weight, spatial_ref, mid_ref, edge_ref, saved_ref, even, odd)


def inner_kernel(
    lead_ref, field_ref, weight_ref, offset_ref, mid_in, edge_in, saved_in,
    mid_ref, edge_ref, saved_ref, even, odd,
):
    @pl.when(lead_ref[0] != 0)
    def _():
        mid_ref[...] = mid_in[...]
        edge_ref[...] = edge_in[...]
        saved_ref[...] = saved_in[...]

    @pl.when(lead_ref[0] == 0)
    def _():
        inner_layers(field_ref, weight_ref, offset_ref, mid_ref, edge_ref, saved_ref, even, odd)


def inner_layers(field_ref, weight_ref, offset_ref, mid_ref, edge_ref, saved_ref, even, odd):
    views, rows, cols, chans = field_ref.shape
    layers = weight_ref.shape[0]
    mid = cols - TILE
    bufs = (even, odd)
    for buf in bufs:
        clear_borders(buf)

    def keep(layer, row, cells):
        saved_ref[layer, row] = cells[:, mid:].reshape(views * TILE, chans).astype(saved_ref.dtype)

    for row in range(rows):
        cells = pltpu.roll(field_ref[:, row].astype(jnp.float32), cols - EDGE, 1)
        put_shifted(even, row + 1, cells)
        keep(0, row, cells)
    for layer in range(layers):
        src, dst = bufs[layer % 2], bufs[(layer + 1) % 2]
        weight = spatial_weight(weight_ref, layer)
        offset = offset_ref[layer : layer + 1]
        for pair in range(rows // 2):
            stacked = jnp.concatenate([src[b, 2 * pair + k] for k in range(4) for b in range(3)], axis=1)
            total = jnp.dot(stacked, weight, preferred_element_type=jnp.float32)
            cells = [
                gelu(total[:, r * chans : (r + 1) * chans] + offset).reshape(views, cols, chans) for r in range(2)
            ]
            if layer == layers - 1:
                part = pl.ds(2 * mid * pair, 2 * mid)
                mid_ref[:, part] = jnp.concatenate([c[:, :mid] for c in cells], axis=1).astype(mid_ref.dtype)
                part = pl.ds(2 * TILE * pair, 2 * TILE)
                edge_ref[:, part] = jnp.concatenate([c[:, mid:] for c in cells], axis=1).astype(edge_ref.dtype)
            else:
                for r in range(2):
                    put_shifted(dst, 2 * pair + r + 1, cells[r])
                    keep(layer + 1, 2 * pair + r, cells[r])


def outer_kernel(
    side_ref, near_ref, rest_ref, far_ref, saved_ref, mid_ref, inner_ref, weight_ref, offset_ref,
    whole_ref, edge_ref, halo, even, odd,
):
    reach, lines, chans = near_ref.shape
    all_views = mid_ref.shape[0]
    rows = lines // all_views
    layers = weight_ref.shape[0]
    bufs = (even, odd)
    groups = even.shape[0]
    views = all_views // groups
    mid = mid_ref.shape[1]
    first = side_ref[0] == 0
    place = lax.broadcasted_iota(jnp.int32, (views, TILE, chans), 1)
    whole_ref[:, :mid] = mid_ref[...]
    for place_at in (0, TILE - 1):
        halo[pl.ds(place_at, lines, stride=TILE)] = jnp.zeros((lines, chans), jnp.float32)
    for c in range(reach):
        near = near_ref[c].astype(jnp.float32) + rest_ref[c].astype(jnp.float32)
        far = far_ref[c].astype(jnp.float32)
        halo[pl.ds(EDGE - reach + c, lines, stride=TILE)] = jnp.where(first, far, near)
        halo[pl.ds(EDGE + c, lines, stride=TILE)] = jnp.where(first, near, far)

    def kept(layer, row, group):
        part = saved_ref[layer, row, group * views * TILE : (group + 1) * views * TILE]
        return part.astype(jnp.float32).reshape(views, TILE, chans)

    def put_windows(dst, row, lower, upper, layer):
        for shift in range(3):
            window = jnp.where(
                place < EDGE,
                pltpu.roll(lower, TILE - 1 - layer - shift, 1),
                pltpu.roll(upper, EDGE - 1 + layer - shift, 1),
            )
            dst[shift, row] = window.reshape(views * TILE, chans).astype(dst.dtype)

    for group in range(groups):
        for buf in bufs:
            clear_borders(buf.at[group])
        for row in range(rows):
            own = kept(0, row, group)
            ends = jnp.stack(
                [
                    halo[(view * rows + row) * TILE : (view * rows + row + 1) * TILE]
                    for view in range(group * views, (group + 1) * views)
                ]
            )
            lower = jnp.where(place < EDGE, ends, own)
            upper = jnp.where(place < EDGE, own, ends)
            put_windows(even.at[group], row + 1, lower, upper, 0)
    for layer in range(layers):
        weight = spatial_weight(weight_ref, layer)
        offset = offset_ref[layer : layer + 1]
        for group in range(groups):
            src, dst = bufs[layer % 2].at[group], bufs[(layer + 1) % 2].at[group]
            stacked = jnp.concatenate(
                [
                    jnp.concatenate([src[b, 2 * pair + k] for pair in range(rows // 2)], axis=0)
                    for k in range(4)
                    for b in range(3)
                ],
                axis=1,
            )
            total = jnp.dot(stacked, weight, preferred_element_type=jnp.float32)
            span = views * TILE
            part = slice(group * views, (group + 1) * views)
            for pair in range(rows // 2):
                values = [
                    gelu(
                        total[pair * span : (pair + 1) * span, r * chans : (r + 1) * chans] + offset
                    ).reshape(views, TILE, chans)
                    for r in range(2)
                ]
                if layer < layers - 1:
                    for r, value in enumerate(values):
                        own = kept(layer + 1, 2 * pair + r, group)
                        lower = jnp.where(place > EDGE + layer, own, pltpu.roll(value, 2 + layer, 1))
                        upper = jnp.where(place < EDGE - 1 - layer, own, pltpu.roll(value, TILE - 2 - layer, 1))
                        put_windows(dst, 2 * pair + r + 1, lower, upper, layer + 1)
                else:
                    block = slice(2 * TILE * pair, 2 * TILE * (pair + 1))
                    own = inner_ref[part, block].astype(jnp.float32)
                    kept_place = (place == 0) | (place == TILE - 1)
                    done = jnp.concatenate(
                        [
                            jnp.where(kept_place, own[:, r * TILE : (r + 1) * TILE], pltpu.roll(value, EDGE, 1))
                            for r, value in enumerate(values)
                        ],
                        axis=1,
                    ).astype(edge_ref.dtype)
                    edge_ref[part, block] = done
                    whole_ref[part, mid + 2 * TILE * pair : mid + 2 * TILE * (pair + 1)] = done


def view_pair(sources, pair, views, blank):
    stacked, weight = [], []
    for load, taps in sources:
        for k in range(4):
            view = 2 * pair + k - 1
            if 0 <= view < views:
                stacked.append(load(view))
                weight.append(
                    jnp.concatenate([taps(k) if k < 3 else blank, taps(k - 1) if k > 0 else blank], axis=1)
                )
    return jnp.dot(
        jnp.concatenate(stacked, axis=1), jnp.concatenate(weight, axis=0), preferred_element_type=jnp.float32
    )


def partial_kernel(side_ref, hidden_ref, lead_ref, rest_ref, edge_ref, weight_ref, offset_ref, out_ref):
    pairs, _, wide = out_ref.shape
    chans = wide // 2
    far_tap = jnp.where(side_ref[0] == 0, 0, 2)
    blank = jnp.zeros((chans, chans), weight_ref.dtype)
    offset = jnp.concatenate([offset_ref[...]] * 2, axis=1)
    sources = (
        (lambda view: hidden_ref[view], lambda k: weight_ref[1, k]),
        (
            lambda view: jnp.concatenate([lead_ref[view] + rest_ref[view], edge_ref[view]], axis=0),
            lambda k: weight_ref[far_tap, k],
        ),
    )
    for pair in range(pairs):
        out_ref[pair] = view_pair(sources, pair, 2 * pairs, blank) + offset


def final_kernel(side_ref, near_ref, partial_ref, weight_ref, field_ref, out_hbm, out, sems):
    views, rows, cols, chans = field_ref.shape
    near_tap = jnp.where(side_ref[0] == 0, 2, 0)
    blank = jnp.zeros((chans, chans), weight_ref.dtype)
    mid = rows * (cols - TILE)
    sources = ((lambda view: near_ref[view], lambda k: weight_ref[near_tap, k]),)
    copies = []
    for pair in range(views // 2):
        total = view_pair(sources, pair, views, blank) + partial_ref[pair]
        for r in range(2):
            view = 2 * pair + r
            angular = total[:, r * chans : (r + 1) * chans].astype(jnp.bfloat16).astype(jnp.float32)
            cells = jnp.concatenate(
                [angular[:mid].reshape(rows, cols - TILE, chans), angular[mid:].reshape(rows, TILE, chans)], axis=1
            )
            out[view] = (field_ref[view].astype(jnp.float32) + pltpu.roll(cells, EDGE, 1)).astype(out.dtype)
        part = pl.ds(2 * pair, 2)
        copies.append(pltpu.make_async_copy(out.at[part], out_hbm.at[part], sems.at[pair]))
        copies[-1].start()
    for copy in copies:
        copy.wait()


def neighbours(starts, count, closed=False):
    pairs = []
    for i in starts:
        if i + 1 < count or closed:
            pairs += [(i, (i + 1) % count), ((i + 1) % count, i)]
    return pairs


def params(mebibytes):
    return pltpu.CompilerParams(vmem_limit_bytes=mebibytes * 2**20)


def local(light_field, spatial_weights, spatial_offsets, angular_weight, angular_offset):
    views, rows, cols, chans = light_field.shape
    lon_count, view_count = lax.axis_size("lon"), lax.axis_size("view")
    lon, view = lax.axis_index("lon"), lax.axis_index("view")
    lead = ((lon == 0) & (view > 0)).astype(jnp.int32)[None]
    lon_side, view_side = lax.rem(lon, 2)[None], lax.rem(view, 2)[None]
    layers = spatial_weights.shape[0]
    half = jnp.bfloat16

    def shaped(*shape):
        return jax.ShapeDtypeStruct(shape, half)

    edges = shaped(layers, views * rows, chans)
    inner_shapes = (
        shaped(views, rows * (cols - TILE), chans),
        shaped(views, rows * TILE, chans),
        shaped(layers, rows, views * TILE, chans),
    )
    biases = [jax.ShapeDtypeStruct(b.shape, jnp.float32) for b in (spatial_offsets, angular_offset[None])]
    inner_scratch = [pltpu.VMEM((3, rows + 2, views * cols, chans), half)] * 2
    in_hbm = lambda array: pltpu.with_memory_space_constraint(array, pltpu.HBM)
    near, far, spatial_bias, angular_bias, *early = pl.pallas_call(
        pack_kernel,
        out_shape=(edges, edges, *biases, *inner_shapes),
        in_specs=[SMEM, SMEM, HBM, HBM, HBM, HBM],
        out_specs=(VMEM,) * 7,
        scratch_shapes=[
            pltpu.VMEM((2, views, rows, TILE, chans), half),
            pltpu.VMEM((2, views * rows * TILE, chans), jnp.float32),
            pltpu.VMEM(light_field.shape, half),
            pltpu.VMEM(spatial_weights.shape, half),
            *inner_scratch,
            pltpu.SemaphoreType.DMA((4,)),
        ],
        compiler_params=params(12),
        cost_estimate=pl.CostEstimate(flops=2 * 10**9, bytes_accessed=10**7, transcendentals=0),
        name="pack",
    )(lon_side, lead, in_hbm(light_field), in_hbm(spatial_weights), in_hbm(spatial_offsets), in_hbm(angular_offset[None]))
    far_views = neighbours(range(1, view_count, 2), view_count)
    rest_views = [
        (line * view_count + i, line * view_count + j) for line in range(1, lon_count) for i, j in far_views
    ]
    near_lead = lax.ppermute(near, "lon", neighbours(range(0, 2, 2), lon_count))
    mid_lead = lax.ppermute(early[0], ("lon", "view"), far_views)
    far = lax.ppermute(far, "lon", neighbours(range(1, lon_count, 2), lon_count, True))
    near_rest = lax.ppermute(near, "lon", neighbours(range(2, lon_count, 2), lon_count))

    mid, edge, saved = pl.pallas_call(
        inner_kernel,
        out_shape=inner_shapes,
        in_specs=[SMEM] + [VMEM] * 6,
        out_specs=(VMEM,) * 3,
        scratch_shapes=inner_scratch,
        compiler_params=params(12),
        name="inner",
    )(lead, light_field, spatial_weights, spatial_bias, *early)
    mid_rest = lax.ppermute(mid, ("lon", "view"), rest_views)
    whole, edge = pl.pallas_call(
        outer_kernel,
        out_shape=(shaped(views, rows * cols, chans), inner_shapes[1]),
        in_specs=[SMEM] + [VMEM] * 8,
        out_specs=(VMEM, VMEM),
        scratch_shapes=[pltpu.VMEM((views * rows * TILE, chans), jnp.float32)]
        + [pltpu.VMEM((GROUPS, 3, rows + 2, views // GROUPS * TILE, chans), half)] * 2,
        compiler_params=params(6),
        name="outer",
    )(lon_side, near_lead, near_rest, far, saved, mid, edge, spatial_weights, spatial_bias)
    far_edge = lax.ppermute(edge, "view", far_views)
    near_rows = lax.ppermute(whole, "view", neighbours(range(0, view_count, 2), view_count))
    partial = pl.pallas_call(
        partial_kernel,
        out_shape=jax.ShapeDtypeStruct((views // 2, rows * cols, 2 * chans), jnp.float32),
        in_specs=[SMEM] + [VMEM] * 6,
        out_specs=VMEM,
        compiler_params=params(6),
        name="partial",
    )(view_side, whole, mid_lead, mid_rest, far_edge, angular_weight, angular_bias)
    return pl.pallas_call(
        final_kernel,
        out_shape=jax.ShapeDtypeStruct(light_field.shape, half),
        in_specs=[SMEM] + [VMEM] * 4,
        out_specs=HBM,
        scratch_shapes=[
            pltpu.VMEM(light_field.shape, half),
            pltpu.SemaphoreType.DMA((views // 2,)),
        ],
        compiler_params=params(6),
        name="final",
    )(view_side, near_rows, partial, angular_weight, light_field)


def solution(mesh):
    return jax.shard_map(
        local,
        mesh=mesh,
        in_specs=(P(("grp", "view"), None, "lon", None), P(), P(), P(), P()),
        out_specs=P(("grp", "view"), None, "lon", None),
        check_vma=False,
    )
```

```python
import jax
import jax.numpy as jnp
from jax import lax
from jax.experimental import pallas as pl
from jax.experimental.pallas import tpu as pltpu
from jax.sharding import PartitionSpec as P


EDGE = 4
TILE = 8
GROUPS = 2
LEAD = 2
LEAD_GROUPS = 1
VMEM = pl.BlockSpec(memory_space=pltpu.VMEM)
SMEM = pl.BlockSpec(memory_space=pltpu.SMEM)
HBM = pl.BlockSpec(memory_space=pl.ANY)


def gelu(t):
    half = 0.5 * t
    return half + half * jnp.tanh(t * (0.7978845608 + (0.7978845608 * 0.044715) * (t * t)))


def pair_weight(block, blank, count):
    return jnp.concatenate(
        [
            jnp.concatenate([block(k, b) if k < 3 else blank, block(k - 1, b) if k > 0 else blank], axis=1)
            for k in range(4)
            for b in range(count)
        ],
        axis=0,
    )


def spatial_weight(weight_ref, layer):
    blank = jnp.zeros(weight_ref.shape[-2:], weight_ref.dtype)
    return pair_weight(lambda k, b: weight_ref[layer, k, b], blank, 3)


def put_shifted(dst, row, cells):
    groups, width, chans = cells.shape
    for shift, moved in ((0, pltpu.roll(cells, 1, 1)), (1, cells), (2, pltpu.roll(cells, width - 1, 1))):
        dst[shift, row] = moved.reshape(groups * width, chans).astype(dst.dtype)


def clear_borders(buf):
    for shift in range(3):
        for row in (0, buf.shape[1] - 1):
            buf[shift, row] = jnp.zeros(buf.shape[2:], buf.dtype)


def take_edges(side_ref, columns, near_ref, far_ref):
    reach, lines, _ = near_ref.shape
    first = side_ref[0] == 0
    for c in range(reach):
        head = columns[0, pl.ds(c, lines, stride=TILE)]
        tail = columns[1, pl.ds(TILE - reach + c, lines, stride=TILE)]
        near_ref[c] = jnp.where(first, tail, head).astype(near_ref.dtype)
        if far_ref is not None:
            far_ref[c] = jnp.where(first, head, tail).astype(far_ref.dtype)


def early_kernel(
    side_ref, lead_ref, field_hbm, weight_hbm, spatial_hbm, angular_hbm,
    near_ref, spatial_ref, angular_ref, mid_ref, edge_ref, saved_ref,
    tiles, columns, field, weight, even, odd, sems,
):
    cols = field_hbm.shape[2]

    @pl.when(lead_ref[0] > 0)
    def _():
        copies = [
            pltpu.make_async_copy(field_hbm.at[:, :, pl.ds(start, TILE)], tiles.at[i], sems.at[i])
            for i, start in enumerate((0, cols - TILE))
        ]
        copies.append(pltpu.make_async_copy(spatial_hbm, spatial_ref, sems.at[2]))
        copies.append(pltpu.make_async_copy(angular_hbm, angular_ref, sems.at[3]))
        for copy in copies:
            copy.start()
        for copy in copies:
            copy.wait()
        for i in range(2):
            columns[i] = tiles[i].astype(jnp.float32).reshape(columns.shape[1:])
        take_edges(side_ref, columns, near_ref, None)

    @pl.when(lead_ref[0] == LEAD)
    def _():
        loads = (
            pltpu.make_async_copy(field_hbm, field, sems.at[0]),
            pltpu.make_async_copy(weight_hbm, weight, sems.at[1]),
        )
        for load in loads:
            load.start()
        for load in loads:
            load.wait()
        inner_layers(field, weight, spatial_ref, mid_ref, edge_ref, saved_ref, even, odd)


def edges_kernel(
    side_ref, lead_ref, field_ref, spatial_ref, first_ref, saved_ref, inner_ref, weight_hbm,
    near_ref, far_ref, edge_ref,
    columns, weight, halo, even, odd, sem,
):
    cols = field_ref.shape[2]
    for i, start in enumerate((0, cols - TILE)):
        columns[i] = field_ref[:, :, start : start + TILE].astype(jnp.float32).reshape(columns.shape[1:])
    take_edges(side_ref, columns, near_ref, far_ref)

    @pl.when(lead_ref[0] == LEAD)
    def _():
        load = pltpu.make_async_copy(weight_hbm, weight, sem)
        load.start()
        load.wait()
        put_halo(halo, first_ref, None, None, None)
        outer_layers("rr", halo, saved_ref, inner_ref, weight, spatial_ref, ((edge_ref, 0),), even, odd, 1)


def inner_kernel(
    lead_ref, field_ref, weight_ref, spatial_in, angular_in, mid_in, edge_in, saved_in, spatial_hbm, angular_hbm,
    mid_ref, edge_ref, saved_ref, spatial_ref, angular_ref, even, odd, sems,
):
    @pl.when(lead_ref[0] > 0)
    def _():
        spatial_ref[...] = spatial_in[...]
        angular_ref[...] = angular_in[...]

    @pl.when(lead_ref[0] == 0)
    def _():
        copies = (
            pltpu.make_async_copy(spatial_hbm, spatial_ref, sems.at[0]),
            pltpu.make_async_copy(angular_hbm, angular_ref, sems.at[1]),
        )
        for copy in copies:
            copy.start()
        for copy in copies:
            copy.wait()

    @pl.when(lead_ref[0] == LEAD)
    def _():
        mid_ref[...] = mid_in[...]
        edge_ref[...] = edge_in[...]
        saved_ref[...] = saved_in[...]

    @pl.when(lead_ref[0] != LEAD)
    def _():
        inner_layers(field_ref, weight_ref, spatial_ref, mid_ref, edge_ref, saved_ref, even, odd)


def inner_layers(field_ref, weight_ref, offset_ref, mid_ref, edge_ref, saved_ref, even, odd):
    views, rows, cols, chans = field_ref.shape
    layers = weight_ref.shape[0]
    mid = cols - TILE
    bufs = (even, odd)
    for buf in bufs:
        clear_borders(buf)

    def keep(layer, row, cells):
        saved_ref[layer, row] = cells[:, mid:].reshape(views * TILE, chans).astype(saved_ref.dtype)

    for row in range(rows):
        cells = pltpu.roll(field_ref[:, row].astype(jnp.float32), cols - EDGE, 1)
        put_shifted(even, row + 1, cells)
        keep(0, row, cells)
    for layer in range(layers):
        src, dst = bufs[layer % 2], bufs[(layer + 1) % 2]
        weight = spatial_weight(weight_ref, layer)
        offset = offset_ref[layer : layer + 1]
        for pair in range(rows // 2):
            stacked = jnp.concatenate([src[b, 2 * pair + k] for k in range(4) for b in range(3)], axis=1)
            total = jnp.dot(stacked, weight, preferred_element_type=jnp.float32)
            cells = [
                gelu(total[:, r * chans : (r + 1) * chans] + offset).reshape(views, cols, chans) for r in range(2)
            ]
            if layer == layers - 1:
                part = pl.ds(2 * mid * pair, 2 * mid)
                mid_ref[:, part] = jnp.concatenate([c[:, :mid] for c in cells], axis=1).astype(mid_ref.dtype)
                part = pl.ds(2 * TILE * pair, 2 * TILE)
                edge_ref[:, part] = jnp.concatenate([c[:, mid:] for c in cells], axis=1).astype(edge_ref.dtype)
            else:
                for r in range(2):
                    put_shifted(dst, 2 * pair + r + 1, cells[r])
                    keep(layer + 1, 2 * pair + r, cells[r])


def put_halo(halo, near_ref, rest_ref, far_ref, first):
    reach, lines, _ = near_ref.shape
    halo[...] = jnp.zeros(halo.shape, halo.dtype)
    for c in range(reach):
        near = near_ref[c].astype(jnp.float32)
        if rest_ref is None:
            halo[pl.ds(EDGE + c, lines, stride=TILE)] = near
            continue
        near = near + rest_ref[c].astype(jnp.float32)
        far = far_ref[c].astype(jnp.float32)
        halo[pl.ds(EDGE - reach + c, lines, stride=TILE)] = jnp.where(first, far, near)
        halo[pl.ds(EDGE + c, lines, stride=TILE)] = jnp.where(first, near, far)


def outer_layers(mode, halo, saved_ref, inner_ref, weight_ref, offset_ref, edge_refs, even, odd, groups):
    layers, rows = saved_ref.shape[:2]
    chans = weight_ref.shape[-1]
    all_views = inner_ref.shape[0]
    views = all_views // groups
    tiles = views if mode == "lr" else views // 2
    width = tiles * TILE
    place = lax.broadcasted_iota(jnp.int32, (tiles, TILE, chans), 1)
    bufs = (even, odd)

    def halves(cells):
        if mode == "lr":
            return cells, cells
        cells = cells.reshape(tiles, 2, TILE, chans)
        return cells[:, 0], cells[:, 1]

    def roll(cells, amount):
        return pltpu.roll(cells, amount % TILE, 1) if amount % TILE else cells

    def kept(layer, row, group):
        part = saved_ref[layer, row, group * views * TILE : (group + 1) * views * TILE]
        return halves(part.astype(jnp.float32).reshape(views, TILE, chans))

    def put_windows(dst, row, bases, layer):
        for shift in range(3):
            taken = [
                roll(base, EDGE * half - (1 + layer + shift if kind == "l" else 1 - layer + shift))
                for half, (kind, base) in enumerate(zip(mode, bases))
            ]
            window = jnp.where(place < EDGE, taken[0], taken[1])
            dst[shift, row, :width] = window.reshape(width, chans).astype(dst.dtype)

    for group in range(groups):
        for buf in bufs:
            clear_borders(buf.at[group])
        for row in range(rows):
            ends = jnp.stack(
                [
                    halo[(view * rows + row) * TILE : (view * rows + row + 1) * TILE]
                    for view in range(group * views, (group + 1) * views)
                ]
            )
            bases = [
                jnp.where((place < EDGE) == (kind == "l"), end, own)
                for kind, end, own in zip(mode, halves(ends), kept(0, row, group))
            ]
            put_windows(even.at[group], row + 1, bases, 0)
    for layer in range(layers):
        weight = spatial_weight(weight_ref, layer)
        offset = offset_ref[layer : layer + 1]
        for group in range(groups):
            src, dst = bufs[layer % 2].at[group], bufs[(layer + 1) % 2].at[group]
            stacked = jnp.concatenate(
                [
                    jnp.concatenate([src[b, 2 * pair + k, :width] for pair in range(rows // 2)], axis=0)
                    for k in range(4)
                    for b in range(3)
                ],
                axis=1,
            )
            total = jnp.dot(stacked, weight, preferred_element_type=jnp.float32)
            for pair in range(rows // 2):
                values = [
                    gelu(
                        total[pair * width : (pair + 1) * width, r * chans : (r + 1) * chans] + offset
                    ).reshape(tiles, TILE, chans)
                    for r in range(2)
                ]
                if layer < layers - 1:
                    for r, value in enumerate(values):
                        bases = []
                        for half, (kind, own) in enumerate(zip(mode, kept(layer + 1, 2 * pair + r, group))):
                            if kind == "l":
                                fresh, keep = roll(value, 2 + layer - EDGE * half), place > EDGE + layer
                            else:
                                fresh, keep = roll(value, 2 - layer - EDGE * half), place < EDGE - 1 - layer
                            bases.append(jnp.where(keep, own, fresh))
                        put_windows(dst, 2 * pair + r + 1, bases, layer + 1)
                    continue
                part = slice(group * views, (group + 1) * views)
                block = inner_ref[part, 2 * TILE * pair : 2 * TILE * (pair + 1)].astype(jnp.float32)
                done = []
                for r, value in enumerate(values):
                    outs = list(halves(block[:, r * TILE : (r + 1) * TILE]))
                    for half, kind in enumerate(mode):
                        if kind == "l":
                            fresh, new = roll(value, EDGE - EDGE * half), (place >= EDGE) & (place < TILE - 1)
                        else:
                            fresh, new = roll(value, -EDGE * half), (place < EDGE) & (place > 0)
                        at = 0 if mode == "lr" else half
                        outs[at] = jnp.where(new, fresh, outs[at])
                    done.append(outs[0] if mode == "lr" else jnp.stack(outs, axis=1).reshape(views, TILE, chans))
                done = jnp.concatenate(done, axis=1)
                for ref, start in edge_refs:
                    ref[part, start + 2 * TILE * pair : start + 2 * TILE * (pair + 1)] = done.astype(ref.dtype)


def outer_kernel(
    side_ref, lead_ref, near_ref, rest_ref, far_ref, saved_ref, mid_ref, inner_ref, weight_ref, offset_ref,
    whole_ref, edge_ref, halo, even, odd,
):
    mid = mid_ref.shape[1]
    whole_ref[:, :mid] = mid_ref[...]
    put_halo(halo, near_ref, rest_ref, far_ref, side_ref[0] == 0)
    results = ((edge_ref, 0), (whole_ref, mid))
    for mode, when, groups in (("ll", lead_ref[0] == LEAD, LEAD_GROUPS), ("lr", lead_ref[0] != LEAD, GROUPS)):

        @pl.when(when)
        def _():
            outer_layers(
                mode, halo, saved_ref, inner_ref, weight_ref, offset_ref, results, even, odd, groups
            )


def view_pair(sources, pair, views, blank):
    stacked, weight = [], []
    for load, taps in sources:
        for k in range(4):
            view = 2 * pair + k - 1
            if 0 <= view < views:
                stacked.append(load(view))
                weight.append(
                    jnp.concatenate([taps(k) if k < 3 else blank, taps(k - 1) if k > 0 else blank], axis=1)
                )
    return jnp.dot(
        jnp.concatenate(stacked, axis=1), jnp.concatenate(weight, axis=0), preferred_element_type=jnp.float32
    )


def partial_kernel(side_ref, hidden_ref, lead_ref, rest_ref, edge_ref, weight_ref, offset_ref, out_ref):
    pairs, _, wide = out_ref.shape
    chans = wide // 2
    far_tap = jnp.where(side_ref[0] == 0, 0, 2)
    blank = jnp.zeros((chans, chans), weight_ref.dtype)
    offset = jnp.concatenate([offset_ref[...]] * 2, axis=1)
    sources = (
        (lambda view: hidden_ref[view], lambda k: weight_ref[1, k]),
        (
            lambda view: jnp.concatenate([lead_ref[view] + rest_ref[view], edge_ref[view]], axis=0),
            lambda k: weight_ref[far_tap, k],
        ),
    )
    for pair in range(pairs):
        out_ref[pair] = view_pair(sources, pair, 2 * pairs, blank) + offset


def final_kernel(side_ref, near_ref, partial_ref, weight_ref, field_ref, out_hbm, out, sems):
    views, rows, cols, chans = field_ref.shape
    near_tap = jnp.where(side_ref[0] == 0, 2, 0)
    blank = jnp.zeros((chans, chans), weight_ref.dtype)
    mid = rows * (cols - TILE)
    sources = ((lambda view: near_ref[view], lambda k: weight_ref[near_tap, k]),)
    copies = []
    for pair in range(views // 2):
        total = view_pair(sources, pair, views, blank) + partial_ref[pair]
        for r in range(2):
            view = 2 * pair + r
            angular = total[:, r * chans : (r + 1) * chans].astype(jnp.bfloat16).astype(jnp.float32)
            cells = jnp.concatenate(
                [angular[:mid].reshape(rows, cols - TILE, chans), angular[mid:].reshape(rows, TILE, chans)], axis=1
            )
            out[view] = (field_ref[view].astype(jnp.float32) + pltpu.roll(cells, EDGE, 1)).astype(out.dtype)
        part = pl.ds(2 * pair, 2)
        copies.append(pltpu.make_async_copy(out.at[part], out_hbm.at[part], sems.at[pair]))
        copies[-1].start()
    for copy in copies:
        copy.wait()


def neighbours(starts, count, closed=False):
    pairs = []
    for i in starts:
        if i + 1 < count or closed:
            pairs += [(i, (i + 1) % count), ((i + 1) % count, i)]
    return pairs


def params(mebibytes):
    return pltpu.CompilerParams(vmem_limit_bytes=mebibytes * 2**20)


def local(light_field, spatial_weights, spatial_offsets, angular_weight, angular_offset):
    views, rows, cols, chans = light_field.shape
    lon_count, view_count = lax.axis_size("lon"), lax.axis_size("view")
    lon, view = lax.axis_index("lon"), lax.axis_index("view")
    lead = ((lon <= 1).astype(jnp.int32) + ((lon == 0) & (view > 0)).astype(jnp.int32))[None]
    lon_side, view_side = lax.rem(lon, 2)[None], lax.rem(view, 2)[None]
    layers = spatial_weights.shape[0]
    half = jnp.bfloat16

    def shaped(*shape):
        return jax.ShapeDtypeStruct(shape, half)

    edges = shaped(layers, views * rows, chans)
    inner_shapes = (
        shaped(views, rows * (cols - TILE), chans),
        shaped(views, rows * TILE, chans),
        shaped(layers, rows, views * TILE, chans),
    )
    biases = [jax.ShapeDtypeStruct(b.shape, jnp.float32) for b in (spatial_offsets, angular_offset[None])]
    inner_scratch = [pltpu.VMEM((3, rows + 2, views * cols, chans), half)] * 2
    in_hbm = lambda array: pltpu.with_memory_space_constraint(array, pltpu.HBM)
    columns = pltpu.VMEM((2, views * rows * TILE, chans), jnp.float32)
    offsets = in_hbm(spatial_offsets), in_hbm(angular_offset[None])
    near_first, spatial_first, angular_first, early_mid, early_edge, early_saved = pl.pallas_call(
        early_kernel,
        out_shape=(edges, *biases, *inner_shapes),
        in_specs=[SMEM, SMEM] + [HBM] * 4,
        out_specs=(VMEM,) * 6,
        scratch_shapes=[
            pltpu.VMEM((2, views, rows, TILE, chans), half),
            columns,
            pltpu.VMEM(light_field.shape, half),
            pltpu.VMEM(spatial_weights.shape, half),
            *inner_scratch,
            pltpu.SemaphoreType.DMA((4,)),
        ],
        compiler_params=params(12),
        cost_estimate=pl.CostEstimate(flops=2 * 10**9, bytes_accessed=10**7, transcendentals=0),
        name="early",
    )(lon_side, lead, in_hbm(light_field), in_hbm(spatial_weights), *offsets)
    far_views = neighbours(range(1, view_count, 2), view_count)
    rest_views = [
        (line * view_count + i, line * view_count + j) for line in range(1, lon_count) for i, j in far_views
    ]
    near_lead = lax.ppermute(near_first, "lon", neighbours(range(0, 2, 2), lon_count))
    mid_lead = lax.ppermute(early_mid, ("lon", "view"), far_views)
    near, far, early_edge = pl.pallas_call(
        edges_kernel,
        out_shape=(edges, edges, inner_shapes[1]),
        in_specs=[SMEM, SMEM] + [VMEM] * 5 + [HBM],
        out_specs=(VMEM,) * 3,
        scratch_shapes=[
            columns,
            pltpu.VMEM(spatial_weights.shape, half),
            pltpu.VMEM((views * rows * TILE, chans), jnp.float32),
            *[pltpu.VMEM((1, 3, rows + 2, views * TILE // 2, chans), half)] * 2,
            pltpu.SemaphoreType.DMA,
        ],
        compiler_params=params(8),
        name="edges",
    )(
        lon_side, lead, light_field, spatial_first, near_lead, early_saved, early_edge, in_hbm(spatial_weights)
    )
    far = lax.ppermute(far, "lon", neighbours(range(1, lon_count, 2), lon_count, True))
    near_rest = lax.ppermute(near, "lon", neighbours(range(2, lon_count, 2), lon_count))

    mid, edge, saved, spatial_bias, angular_bias = pl.pallas_call(
        inner_kernel,
        out_shape=(*inner_shapes, *biases),
        in_specs=[SMEM] + [VMEM] * 7 + [HBM] * 2,
        out_specs=(VMEM,) * 5,
        scratch_shapes=[*inner_scratch, pltpu.SemaphoreType.DMA((2,))],
        compiler_params=params(12),
        name="inner",
    )(
        lead, light_field, spatial_weights, spatial_first, angular_first, early_mid, early_edge, early_saved, *offsets
    )
    mid_rest = lax.ppermute(mid, ("lon", "view"), rest_views)
    whole, edge = pl.pallas_call(
        outer_kernel,
        out_shape=(shaped(views, rows * cols, chans), inner_shapes[1]),
        in_specs=[SMEM, SMEM] + [VMEM] * 8,
        out_specs=(VMEM, VMEM),
        scratch_shapes=[pltpu.VMEM((views * rows * TILE, chans), jnp.float32)]
        + [pltpu.VMEM((GROUPS, 3, rows + 2, views // GROUPS * TILE, chans), half)] * 2,
        compiler_params=params(6),
        name="outer",
    )(lon_side, lead, near_lead, near_rest, far, saved, mid, edge, spatial_weights, spatial_bias)
    far_edge = lax.ppermute(edge, "view", far_views)
    near_rows = lax.ppermute(whole, "view", neighbours(range(0, view_count, 2), view_count))
    partial = pl.pallas_call(
        partial_kernel,
        out_shape=jax.ShapeDtypeStruct((views // 2, rows * cols, 2 * chans), jnp.float32),
        in_specs=[SMEM] + [VMEM] * 6,
        out_specs=VMEM,
        compiler_params=params(6),
        name="partial",
    )(view_side, whole, mid_lead, mid_rest, far_edge, angular_weight, angular_bias)
    return pl.pallas_call(
        final_kernel,
        out_shape=jax.ShapeDtypeStruct(light_field.shape, half),
        in_specs=[SMEM] + [VMEM] * 4,
        out_specs=HBM,
        scratch_shapes=[
            pltpu.VMEM(light_field.shape, half),
            pltpu.SemaphoreType.DMA((views // 2,)),
        ],
        compiler_params=params(6),
        name="final",
    )(view_side, near_rows, partial, angular_weight, light_field)


def solution(mesh):
    return jax.shard_map(
        local,
        mesh=mesh,
        in_specs=(P(("grp", "view"), None, "lon", None), P(), P(), P(), P()),
        out_specs=P(("grp", "view"), None, "lon", None),
        check_vma=False,
    )
```

```python
import jax
import jax.numpy as jnp
from jax import lax
from jax.experimental import pallas as pl
from jax.experimental.pallas import tpu as pltpu
from jax.sharding import PartitionSpec as P


EDGE = 4
TILE = 8
GROUPS = 2
LEAD = 2
VMEM = pl.BlockSpec(memory_space=pltpu.VMEM)
SMEM = pl.BlockSpec(memory_space=pltpu.SMEM)
HBM = pl.BlockSpec(memory_space=pl.ANY)


def gelu(t):
    half = 0.5 * t
    return half + half * jnp.tanh(t * (0.7978845608 + (0.7978845608 * 0.044715) * (t * t)))


def pair_weight(block, blank, count):
    return jnp.concatenate(
        [
            jnp.concatenate([block(k, b) if k < 3 else blank, block(k - 1, b) if k > 0 else blank], axis=1)
            for k in range(4)
            for b in range(count)
        ],
        axis=0,
    )


def spatial_weight(weight_ref, layer):
    blank = jnp.zeros(weight_ref.shape[-2:], weight_ref.dtype)
    return pair_weight(lambda k, b: weight_ref[layer, k, b], blank, 3)


def put_shifted(dst, row, cells):
    groups, width, chans = cells.shape
    for shift, moved in ((0, pltpu.roll(cells, 1, 1)), (1, cells), (2, pltpu.roll(cells, width - 1, 1))):
        dst[shift, row] = moved.reshape(groups * width, chans).astype(dst.dtype)


def clear_borders(buf):
    for shift in range(3):
        for row in (0, buf.shape[1] - 1):
            buf[shift, row] = jnp.zeros(buf.shape[2:], buf.dtype)


def take_edges(side_ref, columns, near_ref, far_ref):
    reach, lines, _ = near_ref.shape
    first = side_ref[0] == 0
    for c in range(reach):
        head = columns[0, pl.ds(c, lines, stride=TILE)]
        tail = columns[1, pl.ds(TILE - reach + c, lines, stride=TILE)]
        near_ref[c] = jnp.where(first, tail, head).astype(near_ref.dtype)
        if far_ref is not None:
            far_ref[c] = jnp.where(first, head, tail).astype(far_ref.dtype)


def early_kernel(
    side_ref, lead_ref, field_hbm, weight_hbm, offset_hbm,
    near_ref, mid_ref, edge_ref, saved_ref,
    tiles, columns, field, weight, offset, even, odd, sems,
):
    cols = field_hbm.shape[2]

    @pl.when(lead_ref[0] > 0)
    def _():
        copies = [
            pltpu.make_async_copy(field_hbm.at[:, :, pl.ds(start, TILE)], tiles.at[i], sems.at[i])
            for i, start in enumerate((0, cols - TILE))
        ]
        for copy in copies:
            copy.start()
        for copy in copies:
            copy.wait()
        for i in range(2):
            columns[i] = tiles[i].astype(jnp.float32).reshape(columns.shape[1:])
        take_edges(side_ref, columns, near_ref, None)

    @pl.when(lead_ref[0] == LEAD)
    def _():
        loads = (
            pltpu.make_async_copy(field_hbm, field, sems.at[0]),
            pltpu.make_async_copy(weight_hbm, weight, sems.at[1]),
            pltpu.make_async_copy(offset_hbm, offset, sems.at[2]),
        )
        for load in loads:
            load.start()
        for load in loads:
            load.wait()
        inner_layers(field, weight, offset, mid_ref, edge_ref, saved_ref, even, odd)


def edges_kernel(side_ref, field_ref, spatial_in, angular_in, near_ref, far_ref, spatial_ref, angular_ref, columns):
    cols = field_ref.shape[2]
    for i, start in enumerate((0, cols - TILE)):
        columns[i] = field_ref[:, :, start : start + TILE].astype(jnp.float32).reshape(columns.shape[1:])
    take_edges(side_ref, columns, near_ref, far_ref)
    spatial_ref[...] = spatial_in[...]
    angular_ref[...] = angular_in[...]


def inner_kernel(
    lead_ref, field_ref, weight_ref, offset_ref, mid_in, edge_in, saved_in,
    mid_ref, edge_ref, saved_ref, even, odd,
):
    @pl.when(lead_ref[0] == LEAD)
    def _():
        mid_ref[...] = mid_in[...]
        edge_ref[...] = edge_in[...]
        saved_ref[...] = saved_in[...]

    @pl.when(lead_ref[0] != LEAD)
    def _():
        inner_layers(field_ref, weight_ref, offset_ref, mid_ref, edge_ref, saved_ref, even, odd)


def inner_layers(field_ref, weight_ref, offset_ref, mid_ref, edge_ref, saved_ref, even, odd):
    views, rows, cols, chans = field_ref.shape
    layers = weight_ref.shape[0]
    mid = cols - TILE
    bufs = (even, odd)
    for buf in bufs:
        clear_borders(buf)

    def keep(layer, row, cells):
        saved_ref[layer, row] = cells[:, mid:].reshape(views * TILE, chans).astype(saved_ref.dtype)

    for row in range(rows):
        cells = pltpu.roll(field_ref[:, row].astype(jnp.float32), cols - EDGE, 1)
        put_shifted(even, row + 1, cells)
        keep(0, row, cells)
    for layer in range(layers):
        src, dst = bufs[layer % 2], bufs[(layer + 1) % 2]
        weight = spatial_weight(weight_ref, layer)
        offset = offset_ref[layer : layer + 1]
        for pair in range(rows // 2):
            stacked = jnp.concatenate([src[b, 2 * pair + k] for k in range(4) for b in range(3)], axis=1)
            total = jnp.dot(stacked, weight, preferred_element_type=jnp.float32)
            cells = [
                gelu(total[:, r * chans : (r + 1) * chans] + offset).reshape(views, cols, chans) for r in range(2)
            ]
            if layer == layers - 1:
                part = pl.ds(2 * mid * pair, 2 * mid)
                mid_ref[:, part] = jnp.concatenate([c[:, :mid] for c in cells], axis=1).astype(mid_ref.dtype)
                part = pl.ds(2 * TILE * pair, 2 * TILE)
                edge_ref[:, part] = jnp.concatenate([c[:, mid:] for c in cells], axis=1).astype(edge_ref.dtype)
            else:
                for r in range(2):
                    put_shifted(dst, 2 * pair + r + 1, cells[r])
                    keep(layer + 1, 2 * pair + r, cells[r])


def outer_kernel(
    side_ref, near_ref, rest_ref, far_ref, saved_ref, mid_ref, inner_ref, weight_ref, offset_ref,
    whole_ref, edge_ref, halo, even, odd,
):
    reach, lines, chans = near_ref.shape
    all_views = mid_ref.shape[0]
    rows = lines // all_views
    layers = weight_ref.shape[0]
    bufs = (even, odd)
    groups = even.shape[0]
    views = all_views // groups
    mid = mid_ref.shape[1]
    first = side_ref[0] == 0
    place = lax.broadcasted_iota(jnp.int32, (views, TILE, chans), 1)
    whole_ref[:, :mid] = mid_ref[...]
    for place_at in (0, TILE - 1):
        halo[pl.ds(place_at, lines, stride=TILE)] = jnp.zeros((lines, chans), jnp.float32)
    for c in range(reach):
        near = near_ref[c].astype(jnp.float32) + rest_ref[c].astype(jnp.float32)
        far = far_ref[c].astype(jnp.float32)
        halo[pl.ds(EDGE - reach + c, lines, stride=TILE)] = jnp.where(first, far, near)
        halo[pl.ds(EDGE + c, lines, stride=TILE)] = jnp.where(first, near, far)

    def kept(layer, row, group):
        part = saved_ref[layer, row, group * views * TILE : (group + 1) * views * TILE]
        return part.astype(jnp.float32).reshape(views, TILE, chans)

    def put_windows(dst, row, lower, upper, layer):
        for shift in range(3):
            window = jnp.where(
                place < EDGE,
                pltpu.roll(lower, TILE - 1 - layer - shift, 1),
                pltpu.roll(upper, EDGE - 1 + layer - shift, 1),
            )
            dst[shift, row] = window.reshape(views * TILE, chans).astype(dst.dtype)

    for group in range(groups):
        for buf in bufs:
            clear_borders(buf.at[group])
        for row in range(rows):
            own = kept(0, row, group)
            ends = jnp.stack(
                [
                    halo[(view * rows + row) * TILE : (view * rows + row + 1) * TILE]
                    for view in range(group * views, (group + 1) * views)
                ]
            )
            lower = jnp.where(place < EDGE, ends, own)
            upper = jnp.where(place < EDGE, own, ends)
            put_windows(even.at[group], row + 1, lower, upper, 0)
    for layer in range(layers):
        weight = spatial_weight(weight_ref, layer)
        offset = offset_ref[layer : layer + 1]
        for group in range(groups):
            src, dst = bufs[layer % 2].at[group], bufs[(layer + 1) % 2].at[group]
            stacked = jnp.concatenate(
                [
                    jnp.concatenate([src[b, 2 * pair + k] for pair in range(rows // 2)], axis=0)
                    for k in range(4)
                    for b in range(3)
                ],
                axis=1,
            )
            total = jnp.dot(stacked, weight, preferred_element_type=jnp.float32)
            span = views * TILE
            part = slice(group * views, (group + 1) * views)
            for pair in range(rows // 2):
                values = [
                    gelu(
                        total[pair * span : (pair + 1) * span, r * chans : (r + 1) * chans] + offset
                    ).reshape(views, TILE, chans)
                    for r in range(2)
                ]
                if layer < layers - 1:
                    for r, value in enumerate(values):
                        own = kept(layer + 1, 2 * pair + r, group)
                        lower = jnp.where(place > EDGE + layer, own, pltpu.roll(value, 2 + layer, 1))
                        upper = jnp.where(place < EDGE - 1 - layer, own, pltpu.roll(value, TILE - 2 - layer, 1))
                        put_windows(dst, 2 * pair + r + 1, lower, upper, layer + 1)
                else:
                    block = slice(2 * TILE * pair, 2 * TILE * (pair + 1))
                    own = inner_ref[part, block].astype(jnp.float32)
                    kept_place = (place == 0) | (place == TILE - 1)
                    done = jnp.concatenate(
                        [
                            jnp.where(kept_place, own[:, r * TILE : (r + 1) * TILE], pltpu.roll(value, EDGE, 1))
                            for r, value in enumerate(values)
                        ],
                        axis=1,
                    ).astype(edge_ref.dtype)
                    edge_ref[part, block] = done
                    whole_ref[part, mid + 2 * TILE * pair : mid + 2 * TILE * (pair + 1)] = done


def view_pair(sources, pair, views, blank):
    stacked, weight = [], []
    for load, taps in sources:
        for k in range(4):
            view = 2 * pair + k - 1
            if 0 <= view < views:
                stacked.append(load(view))
                weight.append(
                    jnp.concatenate([taps(k) if k < 3 else blank, taps(k - 1) if k > 0 else blank], axis=1)
                )
    return jnp.dot(
        jnp.concatenate(stacked, axis=1), jnp.concatenate(weight, axis=0), preferred_element_type=jnp.float32
    )


def partial_kernel(side_ref, hidden_ref, lead_ref, rest_ref, edge_ref, weight_ref, offset_ref, out_ref):
    pairs, _, wide = out_ref.shape
    chans = wide // 2
    far_tap = jnp.where(side_ref[0] == 0, 0, 2)
    blank = jnp.zeros((chans, chans), weight_ref.dtype)
    offset = jnp.concatenate([offset_ref[...]] * 2, axis=1)
    sources = (
        (lambda view: hidden_ref[view], lambda k: weight_ref[1, k]),
        (
            lambda view: jnp.concatenate([lead_ref[view] + rest_ref[view], edge_ref[view]], axis=0),
            lambda k: weight_ref[far_tap, k],
        ),
    )
    for pair in range(pairs):
        out_ref[pair] = view_pair(sources, pair, 2 * pairs, blank) + offset


def final_kernel(side_ref, near_ref, partial_ref, weight_ref, field_ref, out_hbm, out, sems):
    views, rows, cols, chans = field_ref.shape
    near_tap = jnp.where(side_ref[0] == 0, 2, 0)
    blank = jnp.zeros((chans, chans), weight_ref.dtype)
    mid = rows * (cols - TILE)
    sources = ((lambda view: near_ref[view], lambda k: weight_ref[near_tap, k]),)
    copies = []
    for pair in range(views // 2):
        total = view_pair(sources, pair, views, blank) + partial_ref[pair]
        for r in range(2):
            view = 2 * pair + r
            angular = total[:, r * chans : (r + 1) * chans].astype(jnp.bfloat16).astype(jnp.float32)
            cells = jnp.concatenate(
                [angular[:mid].reshape(rows, cols - TILE, chans), angular[mid:].reshape(rows, TILE, chans)], axis=1
            )
            out[view] = (field_ref[view].astype(jnp.float32) + pltpu.roll(cells, EDGE, 1)).astype(out.dtype)
        part = pl.ds(2 * pair, 2)
        copies.append(pltpu.make_async_copy(out.at[part], out_hbm.at[part], sems.at[pair]))
        copies[-1].start()
    for copy in copies:
        copy.wait()


def neighbours(starts, count, closed=False):
    pairs = []
    for i in starts:
        if i + 1 < count or closed:
            pairs += [(i, (i + 1) % count), ((i + 1) % count, i)]
    return pairs


def params(mebibytes):
    return pltpu.CompilerParams(vmem_limit_bytes=mebibytes * 2**20)


def local(light_field, spatial_weights, spatial_offsets, angular_weight, angular_offset):
    views, rows, cols, chans = light_field.shape
    lon_count, view_count = lax.axis_size("lon"), lax.axis_size("view")
    lon, view = lax.axis_index("lon"), lax.axis_index("view")
    lead = ((lon <= 1).astype(jnp.int32) + ((lon == 0) & (view > 0)).astype(jnp.int32))[None]
    lon_side, view_side = lax.rem(lon, 2)[None], lax.rem(view, 2)[None]
    layers = spatial_weights.shape[0]
    half = jnp.bfloat16

    def shaped(*shape):
        return jax.ShapeDtypeStruct(shape, half)

    edges = shaped(layers, views * rows, chans)
    inner_shapes = (
        shaped(views, rows * (cols - TILE), chans),
        shaped(views, rows * TILE, chans),
        shaped(layers, rows, views * TILE, chans),
    )
    biases = [jax.ShapeDtypeStruct(b.shape, jnp.float32) for b in (spatial_offsets, angular_offset[None])]
    inner_scratch = [pltpu.VMEM((3, rows + 2, views * cols, chans), half)] * 2
    in_hbm = lambda array: pltpu.with_memory_space_constraint(array, pltpu.HBM)
    columns = pltpu.VMEM((2, views * rows * TILE, chans), jnp.float32)
    near_first, *early = pl.pallas_call(
        early_kernel,
        out_shape=(edges, *inner_shapes),
        in_specs=[SMEM, SMEM, HBM, HBM, HBM],
        out_specs=(VMEM,) * 4,
        scratch_shapes=[
            pltpu.VMEM((2, views, rows, TILE, chans), half),
            columns,
            pltpu.VMEM(light_field.shape, half),
            pltpu.VMEM(spatial_weights.shape, half),
            pltpu.VMEM(spatial_offsets.shape, jnp.float32),
            *inner_scratch,
            pltpu.SemaphoreType.DMA((3,)),
        ],
        compiler_params=params(12),
        cost_estimate=pl.CostEstimate(flops=2 * 10**9, bytes_accessed=10**7, transcendentals=0),
        name="early",
    )(lon_side, lead, in_hbm(light_field), in_hbm(spatial_weights), in_hbm(spatial_offsets))
    near, far, spatial_bias, angular_bias = pl.pallas_call(
        edges_kernel,
        out_shape=(edges, edges, *biases),
        in_specs=[SMEM, VMEM, VMEM, VMEM],
        out_specs=(VMEM,) * 4,
        scratch_shapes=[columns],
        compiler_params=params(4),
        name="edges",
    )(lon_side, light_field, spatial_offsets, angular_offset[None])
    far_views = neighbours(range(1, view_count, 2), view_count)
    rest_views = [
        (line * view_count + i, line * view_count + j) for line in range(1, lon_count) for i, j in far_views
    ]
    near_lead = lax.ppermute(near_first, "lon", neighbours(range(0, 2, 2), lon_count))
    mid_lead = lax.ppermute(early[0], ("lon", "view"), far_views)
    far = lax.ppermute(far, "lon", neighbours(range(1, lon_count, 2), lon_count, True))
    near_rest = lax.ppermute(near, "lon", neighbours(range(2, lon_count, 2), lon_count))

    mid, edge, saved = pl.pallas_call(
        inner_kernel,
        out_shape=inner_shapes,
        in_specs=[SMEM] + [VMEM] * 6,
        out_specs=(VMEM,) * 3,
        scratch_shapes=inner_scratch,
        compiler_params=params(12),
        name="inner",
    )(lead, light_field, spatial_weights, spatial_bias, *early)
    mid_rest = lax.ppermute(mid, ("lon", "view"), rest_views)
    whole, edge = pl.pallas_call(
        outer_kernel,
        out_shape=(shaped(views, rows * cols, chans), inner_shapes[1]),
        in_specs=[SMEM] + [VMEM] * 8,
        out_specs=(VMEM, VMEM),
        scratch_shapes=[pltpu.VMEM((views * rows * TILE, chans), jnp.float32)]
        + [pltpu.VMEM((GROUPS, 3, rows + 2, views // GROUPS * TILE, chans), half)] * 2,
        compiler_params=params(6),
        name="outer",
    )(lon_side, near_lead, near_rest, far, saved, mid, edge, spatial_weights, spatial_bias)
    far_edge = lax.ppermute(edge, "view", far_views)
    near_rows = lax.ppermute(whole, "view", neighbours(range(0, view_count, 2), view_count))
    partial = pl.pallas_call(
        partial_kernel,
        out_shape=jax.ShapeDtypeStruct((views // 2, rows * cols, 2 * chans), jnp.float32),
        in_specs=[SMEM] + [VMEM] * 6,
        out_specs=VMEM,
        compiler_params=params(6),
        name="partial",
    )(view_side, whole, mid_lead, mid_rest, far_edge, angular_weight, angular_bias)
    return pl.pallas_call(
        final_kernel,
        out_shape=jax.ShapeDtypeStruct(light_field.shape, half),
        in_specs=[SMEM] + [VMEM] * 4,
        out_specs=HBM,
        scratch_shapes=[
            pltpu.VMEM(light_field.shape, half),
            pltpu.SemaphoreType.DMA((views // 2,)),
        ],
        compiler_params=params(6),
        name="final",
    )(view_side, near_rows, partial, angular_weight, light_field)


def solution(mesh):
    return jax.shard_map(
        local,
        mesh=mesh,
        in_specs=(P(("grp", "view"), None, "lon", None), P(), P(), P(), P()),
        out_specs=P(("grp", "view"), None, "lon", None),
        check_vma=False,
    )
```
